16 devices in a mesh: rep: 1, dp: 16 (over x, y, z, core).
Axes of the slice: x: 2, y: 2, z: 2, core: 2. Of those that a mesh axis runs over, the one named last changes fastest.
Arguments:
- x: bfloat16 [16, 2048, 1024], P(('rep', 'dp'))
- dy: bfloat16 [16, 2048, 1024], P(('rep', 'dp'))
- wq: bfloat16 [2, 1024, 1024], P(None, 'dp')
- wk: bfloat16 [2, 1024, 1024], P(None, 'dp')
- wv: bfloat16 [2, 1024, 1024], P(None, 'dp')
- wo: bfloat16 [2, 1024, 1024], P(None, 'dp')
- w_gate: bfloat16 [2, 1024, 4096], P(None, 'dp')
- w_up: bfloat16 [2, 1024, 4096], P(None, 'dp')
- w_down: bfloat16 [2, 4096, 1024], P(None, 'dp')
- m_wq: float32 [2, 1024, 1024], P(None, 'dp')
- m_wk: float32 [2, 1024, 1024], P(None, 'dp')
- m_wv: float32 [2, 1024, 1024], P(None, 'dp')
- m_wo: float32 [2, 1024, 1024], P(None, 'dp')
- m_w_gate: float32 [2, 1024, 4096], P(None, 'dp')
- m_w_up: float32 [2, 1024, 4096], P(None, 'dp')
- m_w_down: float32 [2, 4096, 1024], P(None, 'dp')
- v_wq: float32 [2, 1024, 1024], P(None, 'dp')
- v_wk: float32 [2, 1024, 1024], P(None, 'dp')
- v_wv: float32 [2, 1024, 1024], P(None, 'dp')
- v_wo: float32 [2, 1024, 1024], P(None, 'dp')
- v_w_gate: float32 [2, 1024, 4096], P(None, 'dp')
- v_w_up: float32 [2, 1024, 4096], P(None, 'dp')
- v_w_down: float32 [2, 4096, 1024], P(None, 'dp')
Outputs:
- output 1: bfloat16 [2, 1024, 1024], P('rep', 'dp')
- output 2: bfloat16 [2, 1024, 1024], P('rep', 'dp')
- output 3: bfloat16 [2, 1024, 1024], P('rep', 'dp')
- output 4: bfloat16 [2, 1024, 1024], P('rep', 'dp')
- output 5: bfloat16 [2, 1024, 4096], P('rep', 'dp')
- output 6: bfloat16 [2, 1024, 4096], P('rep', 'dp')
- output 7: bfloat16 [2, 4096, 1024], P('rep', 'dp')
- output 8: float32 [2, 1024, 1024], P('rep', 'dp')
- output 9: float32 [2, 1024, 1024], P('rep', 'dp')
- output 10: float32 [2, 1024, 1024], P('rep', 'dp')
- output 11: float32 [2, 1024, 1024], P('rep', 'dp')
- output 12: float32 [2, 1024, 4096], P('rep', 'dp')
- output 13: float32 [2, 1024, 4096], P('rep', 'dp')
- output 14: float32 [2, 4096, 1024], P('rep', 'dp')
- output 15: float32 [2, 1024, 1024], P('rep', 'dp')
- output 16: float32 [2, 1024, 1024], P('rep', 'dp')
- output 17: float32 [2, 1024, 1024], P('rep', 'dp')
- output 18: float32 [2, 1024, 1024], P('rep', 'dp')
- output 19: float32 [2, 1024, 4096], P('rep', 'dp')
- output 20: float32 [2, 1024, 4096], P('rep', 'dp')
- output 21: float32 [2, 4096, 1024], P('rep', 'dp')
All inputs are finite; a program needn't handle non-finite values.
Results may differ from the reference program's by a relative error of at most 0.0248.
Values are sent between devices in bfloat16 or wider.
A program may use at most 2 GiB of HBM per device.

```python
import jax
import jax.numpy as jnp
from jax import lax

SEQUENCES = 16
TOKENS = 2048
D = 1024
HEADS = 4
KV_HEADS = 4
HEAD = 256
FF = 4096
LAYERS = 2
THETA = 10000
NAMES = ("wq", "wk", "wv", "wo", "w_gate", "w_up", "w_down")
SHAPES = {
    "wq": (LAYERS, D, HEADS * HEAD),
    "wk": (LAYERS, D, KV_HEADS * HEAD),
    "wv": (LAYERS, D, KV_HEADS * HEAD),
    "wo": (LAYERS, HEADS * HEAD, D),
    "w_gate": (LAYERS, D, FF),
    "w_up": (LAYERS, D, FF),
    "w_down": (LAYERS, FF, D),
}


def bump(key, n, height):
    away = (jnp.arange(n, dtype=jnp.int32) - jax.random.randint(key, (), 0, n, jnp.int32)) % n
    return jnp.where(away < n // 8, height, 1.0)


def together(key, own, strength):
    shared = jax.random.normal(key, own.shape[1:], jnp.float32)
    return (own + strength * shared) * lax.rsqrt(1 + strength * strength)


def setup_inputs(seed: int = 0, part: int = 0) -> dict:
    kx, kdy, ka, kb, kz, kf, kh, kl, *keys = jax.random.split(jax.random.key(seed), 8 + 3 * len(NAMES))
    kx, kdy, ka, kb = (jax.random.fold_in(k, part) for k in (kx, kdy, ka, kb))
    kw, km, kv = (keys[i::3] for i in range(3))
    shape = (SEQUENCES, TOKENS, D)
    much_x, much_dy = jax.random.uniform(kz, (2,), jnp.float32, 0.0, 1.0)
    loud = 2.0 ** jax.random.uniform(jax.random.fold_in(kz, 1), (), jnp.float32, -1.0, 2.0)
    layers = 2.0 ** jax.random.uniform(kl, (LAYERS, 1, 1), jnp.float32, -1.0, 1.0)
    times = {"wq": 1.0, "wk": 1.0, "wv": 2.0, "wo": layers, "w_gate": 1.0, "w_up": bump(kh, FF, 4.0), "w_down": layers}
    x = together(ka, jax.random.normal(kx, shape, jnp.float32), much_x) * bump(kf, D, 4.0)
    dy = together(kb, jax.random.normal(kdy, shape, jnp.float32), much_dy)
    drawn = {"x": x.astype(jnp.bfloat16), "dy": (loud * dy * (SEQUENCES * TOKENS) ** -0.5).astype(jnp.bfloat16)}
    for key, name in zip(kw, NAMES, strict=True):
        drawn[name] = (jax.random.normal(key, SHAPES[name], jnp.float32) * SHAPES[name][1] ** -0.5 * times[name]).astype(jnp.bfloat16)
    for key, name in zip(km, NAMES, strict=True):
        drawn[f"m_{name}"] = 0.1 * jax.random.normal(key, SHAPES[name], jnp.float32)
    for key, name in zip(kv, NAMES, strict=True):
        drawn[f"v_{name}"] = jax.random.uniform(key, SHAPES[name], jnp.float32, 0.02, 0.06)
    return drawn


def matmul(a, w):
    return jnp.dot(a, w, preferred_element_type=jnp.float32).astype(jnp.bfloat16)


def normed(h):
    wide = h.astype(jnp.float32)
    scale = lax.rsqrt(jnp.mean(wide**2, -1, keepdims=True) + 1e-6)
    return (wide * scale).astype(jnp.bfloat16)


def turned(t, theta):
    half = t.shape[-1] // 2
    angle = jnp.arange(t.shape[0], dtype=jnp.float32)[:, None] * theta ** (-jnp.arange(half, dtype=jnp.float32) / half)
    cos, sin = jnp.cos(angle)[:, None], jnp.sin(angle)[:, None]
    a, b = t[..., :half].astype(jnp.float32), t[..., half:].astype(jnp.float32)
    return jnp.concatenate([a * cos - b * sin, b * cos + a * sin], -1).astype(jnp.bfloat16)


def seen_by(q, k, v):
    tokens, kv = q.shape[0], k.shape[1]
    q = q.reshape(tokens, kv, -1, q.shape[-1])
    scores = jnp.einsum("tgsd,ugd->gstu", q.astype(jnp.float32), k.astype(jnp.float32)) * q.shape[-1] ** -0.5
    place = jnp.arange(tokens)
    weights = jax.nn.softmax(jnp.where(place[:, None] >= place, scores, -jnp.inf), -1).astype(jnp.bfloat16)
    return jnp.einsum("gstu,ugd->tgsd", weights.astype(jnp.float32), v.astype(jnp.float32)).astype(jnp.bfloat16).reshape(tokens, -1)


def layer(h, w):
    a = normed(h)
    q, k = (turned(matmul(a, w[name]).reshape(h.shape[0], -1, HEAD), THETA) for name in ("wq", "wk"))
    h = h + matmul(seen_by(q, k, matmul(a, w["wv"]).reshape(h.shape[0], -1, HEAD)), w["wo"])
    b = normed(h)
    gate = jnp.dot(b, w["w_gate"], preferred_element_type=jnp.float32)
    up = jnp.dot(b, w["w_up"], preferred_element_type=jnp.float32)
    return h + matmul((jax.nn.silu(gate) * up).astype(jnp.bfloat16), w["w_down"])


def adamw(w, m, v, g):
    m = 0.9 * m + 0.1 * g
    v = 0.95 * v + 0.05 * g * g
    step = m * lax.rsqrt(v + 1e-8) + 0.1 * w
    return (w - 0.02 * step).astype(jnp.bfloat16), m, v


def clipped(gradients, sum_of_squares, count):
    factor = jnp.minimum(1.0, 0.5 * lax.rsqrt(sum_of_squares / count + 1e-30))
    return [g * factor for g in gradients]


def stack(weights, h):
    return lax.scan(lambda h, w: (layer(h, w), None), h, weights)[0]


def reference(x, dy, wq, wk, wv, wo, w_gate, w_up, w_down, m_wq, m_wk, m_wv, m_wo, m_w_gate, m_w_up, m_w_down, v_wq, v_wk, v_wv, v_wo, v_w_gate, v_w_up, v_w_down):
    weights = dict(zip(NAMES, (wq, wk, wv, wo, w_gate, w_up, w_down), strict=True))

    def take(so_far, sequence):
        h, by_y = sequence
        _, back = jax.vjp(stack, weights, h)
        by_weights, by_h = back(by_y)
        return jax.tree.map(lambda total, term: total + term.astype(jnp.float32), so_far, by_weights), by_h

    none_yet = {name: jnp.zeros(w.shape, jnp.float32) for name, w in weights.items()}
    by_weights, by_x = lax.scan(take, none_yet, (x, dy))
    gradients = [by_weights[name].astype(jnp.bfloat16).astype(jnp.float32) for name in NAMES]
    gradients = clipped(gradients, sum(jnp.sum(g * g) for g in gradients), sum(g.size for g in gradients))
    first = (m_wq, m_wk, m_wv, m_wo, m_w_gate, m_w_up, m_w_down)
    second = (v_wq, v_wk, v_wv, v_wo, v_w_gate, v_w_up, v_w_down)
    new = [adamw(weights[name].astype(jnp.float32), m, v, g) for name, m, v, g in zip(NAMES, first, second, gradients, strict=True)]
    return tuple(one[which] for which in range(3) for one in new)
```

```python
import jax
import jax.numpy as jnp
from jax import lax
from jax.experimental import pallas as pl
from jax.experimental.pallas import tpu as pltpu
from jax.sharding import PartitionSpec as P

F32, BF16 = jnp.float32, jnp.bfloat16
MESH = pl.DeviceIdType.MESH
ANY = pl.BlockSpec(memory_space=pl.ANY)
DMA, VM = pltpu.SemaphoreType.DMA, pltpu.VMEM
LIMIT = 62 * 2**20
HEAD = 256
HEADS = 4
THETA = 10000
LOG2E = 1.4426950408889634
NEG = -1e30
HIDDEN = 2 * NEG
DIMS = (8, 4, 2)
CORE = 1
ALL = slice(None)
EACH = range(3)
CUBE = (2, 2, 2, 2)


def dot(a, b, ca, cb):
    return lax.dot_general(a, b, (((ca,), (cb,)), ((), ())), preferred_element_type=F32)


def nn(a, b):
    return dot(a, b, 1, 0)


def nt(a, b):
    return dot(a, b, 1, 1)


def tt(a, b):
    return dot(a, b, 0, 0)


def shape(*size, dtype=BF16):
    return jax.ShapeDtypeStruct(size, dtype)


def chunk(n, size):
    return pl.ds(pl.multiple_of(n * size, size), size)


def loop(count, what):
    lax.fori_loop(0, count, lambda n, _: what(n), None)


def bit(mask):
    return lax.rem(lax.axis_index("dp") // mask, 2)


def peer(mask):
    at = lax.axis_index("dp")
    for m in (*DIMS, CORE):
        if mask & m:
            at = at + m - 2 * m * bit(m)
    return {"dp": at}


def place():
    return [bit(m) for m in DIMS]


def among(p, at):
    return tuple(at if n == p else ALL for n in EACH)


def parts_of(arrays):
    size = arrays[0].shape[-1]
    if len(arrays) > 1:
        return [(n, pl.ds(0, size)) for n in EACH]
    unit = size // 128
    wide = -(-unit // 3)
    return [(0, pl.ds(128 * wide * n, 128 * min(wide, unit - wide * n))) for n in EACH]


def remote(src, dst, sems, n, mask):
    return pltpu.make_async_remote_copy(src_ref=src, dst_ref=dst, send_sem=sems[0].at[n], recv_sem=sems[1].at[n], device_id=peer(mask), device_id_type=MESH)


def local(src, dst, sems, n):
    return pltpu.make_async_copy(src, dst, sems.at[n])


def start_all(copies):
    for c in copies:
        c.start()


def wait_all(copies):
    for c in copies:
        c.wait()


def flat(ref):
    size = 1
    for n in ref.shape[:-1]:
        size *= n
    return ref.reshape(size, ref.shape[-1])


def added(into, others, size=64):
    into, others = flat(into), [flat(o) for o in others]

    def some(n):
        at = chunk(n, size)
        total = into[at, :].astype(F32)
        for o in others:
            total = total + o[at, :].astype(F32)
        into[at, :] = total.astype(BF16)

    loop(into.shape[0] // size, some)


class Fetch:
    masks = (*DIMS, CORE)

    def __init__(self, ws, layer, at=(1, 3, 5, 7)):
        _, self.rows, self.columns = ws[0].shape
        self.layer, self.at, self.ins, k = layer, at, list(ws), len(ws)
        self.outs = [shape(*CUBE, self.rows, self.columns)] * k
        self.scratch = [VM((k, self.rows, self.columns), BF16), DMA((2 * k,)), DMA((21,)), DMA((21,))]
        self.parts = parts_of(ws)

    def done(self, outs):
        return [o.reshape(16 * self.rows, self.columns) for o in outs]

    def stages(self, ws, fulls, scratch):
        own, sem, *sems = scratch
        b, core, k = place(), bit(CORE), len(ws)
        loads = lambda: [local(w.at[self.layer], own.at[n], sem, n) for n, w in enumerate(ws)]
        keeps = lambda: [local(own.at[n], full.at[(*b, core)], sem, k + n) for n, full in enumerate(fulls)]
        axis = lambda p, level: (p + 2 - level) % 3

        def held(p, level, other=None):
            which, columns = self.parts[p]
            idx = list(b)
            for n in range(level):
                idx[axis(p, n)] = ALL
            if other:
                idx[axis(p, level)] = 1 - b[axis(p, level)]
            return fulls[which].at[(*idx, core, ALL, columns)]

        def first_of(p):
            which, columns = self.parts[p]
            return own.at[which, :, columns]

        def across(p, level):
            return remote(held(p, level) if level else first_of(p), held(p, level), sems, 3 * level + p, DIMS[axis(p, level)])

        def pair(p, level):
            if not level:
                return remote(first_of(p), held(p, level), sems, 9 + p, CORE)
            got = held(p, level - 1, True)
            return remote(got, got, sems, 9 + 3 * level + p, CORE)

        def begin():
            start_all(loads())

        def first():
            wait_all(loads())
            start_all(keeps())
            start_all([across(p, 0) for p in EACH] + [pair(p, 0) for p in EACH])

        def next_of(level):
            def go():
                if level == 1:
                    wait_all(keeps())
                for p in EACH:
                    across(p, level - 1).wait_recv()
                    if level < 3:
                        across(p, level).start()
                    pair(p, level).start()

            return go

        def end():
            for p in EACH:
                for level in EACH:
                    across(p, level).wait_send()
                wait_all([pair(p, level) for level in range(4)])

        return [(0, begin), *zip(self.at, (first, *(next_of(n + 1) for n in EACH))), (None, end)]


def cube(g):
    return g.reshape(*CUBE, g.shape[0] // 16, g.shape[1])


class Pair:
    masks = (CORE,)

    def __init__(self, grads):
        self.ins = [cube(g) for g in grads]
        self.outs = [shape(*CUBE[1:], *g.shape[4:]) for g in self.ins]
        self.scratch = [DMA((len(grads),))] * 2

    def done(self, outs):
        return outs

    def stages(self, ins, outs, sems):
        copies = lambda: [remote(g.at[:, :, :, 1 - bit(CORE)], r, sems, n, CORE) for n, (g, r) in enumerate(zip(ins, outs))]
        return [(1, lambda: start_all(copies())), (None, lambda: wait_all(copies()))]


class Half:
    masks = DIMS

    def __init__(self, grads, pairs, at=(0, 1, 2)):
        self.at, self.n, self.parts = at, len(grads), parts_of(grads)
        self.ins = [*map(cube, grads), *pairs]
        self.sizes = [(2, 2, self.ins[0].shape[4], c.size) for _, c in self.parts]
        self.outs = [shape(*s) for s in self.sizes]
        self.scratch = [VM(s, BF16) for s in self.sizes] * 2 + [DMA((6,)), DMA((3,)), DMA((3,))]

    def done(self, outs):
        return outs

    def stages(self, ins, outs, scratch):
        grads, pairs = ins[: self.n], ins[self.n :]
        a, r, (sem, *sems) = scratch[:3], scratch[3:6], scratch[6:]

        def loads():
            got = []
            for p, (n, columns) in enumerate(self.parts):
                at = among(p, 1 - bit(DIMS[p]))
                got.append(local(grads[n].at[(*at, bit(CORE), ALL, columns)], a[p], sem, p))
                got.append(local(pairs[n].at[(*at, ALL, columns)], r[p], sem, 3 + p))
            return got

        def add():
            wait_all(loads())
            for p in EACH:
                added(a[p], [r[p]])

        copies = lambda: [remote(a[p], outs[p], sems, p, DIMS[p]) for p in EACH]
        return [*zip(self.at, (lambda: start_all(loads()), add, lambda: start_all(copies()))), (None, lambda: wait_all(copies()))]


class Quad:
    masks = (2, 4, 6, 8, 10, 12)

    def __init__(self, grads, pairs, halves, at=(0, 1, 2)):
        self.at, self.n, self.parts = at, len(grads), parts_of(grads)
        self.ins = [*map(cube, grads), *pairs, *halves]
        rows = self.ins[0].shape[4]
        self.outs = [shape(rows, c.size, dtype=F32) for _, c in self.parts] + [shape(3, rows, c.size) for _, c in self.parts]
        self.scratch = [VM((2, 2, rows, c.size), BF16) for _, c in self.parts] * 3 + [VM((rows, c.size), F32) for _, c in self.parts]
        self.scratch += [DMA((12,)), DMA((9,)), DMA((9,))]

    def done(self, outs):
        return [(*part, *sums) for part, *sums in zip(self.parts, outs[:3], outs[3:])]

    def stages(self, ins, outs, scratch):
        n = self.n
        grads, pairs, halves = ins[:n], ins[n : 2 * n], ins[2 * n :]
        (a, r, s, own), (sem, *sems) = [scratch[3 * i : 3 * i + 3] for i in range(4)], scratch[12:]

        def loads():
            got = []
            for p, (n, columns) in enumerate(self.parts):
                at = among(p, bit(DIMS[p]))
                got.append(local(grads[n].at[(*at, bit(CORE), ALL, columns)], a[p], sem, p))
                got.append(local(pairs[n].at[(*at, ALL, columns)], r[p], sem, 3 + p))
                got.append(local(halves[p], s[p], sem, 6 + p))
            return got

        def add():
            wait_all(loads())
            for p in EACH:
                total_of(p, own[p], a[p], r[p], s[p])
                added(a[p], [r[p], s[p]])

        copies = lambda: [local(own[p], outs[p], sem, 9 + p) for p in EACH] + [c for p in EACH for c in to_three(p, a[p], outs[3 + p], sems)]
        return [*zip(self.at, (lambda: start_all(loads()), add, lambda: start_all(copies()))), (None, lambda: wait_all(copies()))]


def sides(p):
    u, v = (n for n in EACH if n != p)
    return u, v, bit(DIMS[u]), bit(DIMS[v])


def total_of(p, own, *terms, size=64):
    _, _, bu, bv = sides(p)

    def some(n):
        at = chunk(n, size)
        own[at, :] = sum(x[bu, bv, at, :].astype(F32) for x in terms)

    loop(own.shape[0] // size, some)


def to_three(p, blocks, others, sems, base=0):
    u, v, bu, bv = sides(p)
    flips = ((1, 0), (0, 1), (1, 1))
    return [remote(blocks.at[1 - bu if fu else bu, 1 - bv if fv else bv], others.at[n], sems, base + 3 * p + n, DIMS[u] * fu + DIMS[v] * fv)
            for n, (fu, fv) in enumerate(flips)]


IDS = []


def talk():
    IDS.append(None)
    return dict(collective_id=len(IDS), has_side_effects=True)


def hello(masks):
    for m in masks:
        pl.semaphore_signal(pltpu.get_barrier_semaphore(), inc=1, device_id=peer(m), device_id_type=MESH)


def met(masks):
    pl.semaphore_wait(pltpu.get_barrier_semaphore(), len(masks))


def run(body, grid, args, in_specs, out_specs, out_shapes, scratch=(), jobs=(), flops=0):
    steps = 1
    for g in grid:
        steps *= g
    gather = lambda name: [x for job in jobs for x in getattr(job, name)]
    ins, outs, scr = gather("ins"), gather("outs"), gather("scratch")
    masks = sorted(set(gather("masks")))

    def kernel(*refs):
        refs = list(refs)
        take = lambda held, n: [held.pop(0) for _ in range(n)]
        my_in, job_in, my_out, job_out, my_scr, job_scr = (take(refs, len(x)) for x in (args, ins, out_shapes, outs, scratch, scr))
        step = 0
        for axis, g in enumerate(grid):
            step = step * g + pl.program_id(axis)
        plan = {}
        for job in jobs:
            for at, what in job.stages(take(job_in, len(job.ins)), take(job_out, len(job.outs)), take(job_scr, len(job.scratch))):
                plan.setdefault(at if at is None else min(at, steps - 1), []).append(what)
        last = plan.pop(None, [])
        if jobs:
            plan.setdefault(0, []).insert(0, lambda: hello(masks))
            greet = min(1, steps - 1)
            plan.setdefault(greet, []).insert(1 - greet, lambda: met(masks))
        for at in sorted(plan):

            @pl.when(step == at)
            def _(todo=plan[at]):
                for what in todo:
                    what()

        if body is not None:
            body(*my_in, *my_out, *my_scr)
        if last:

            @pl.when(step == steps - 1)
            def _():
                for what in last:
                    what()

    got = list(pl.pallas_call(
        kernel,
        grid=grid,
        in_specs=[*in_specs, *[ANY] * len(ins)],
        out_specs=[*out_specs, *[ANY] * len(outs)],
        out_shape=[*out_shapes, *outs],
        scratch_shapes=[*scratch, *scr],
        compiler_params=pltpu.CompilerParams(dimension_semantics=("arbitrary",) * len(grid), vmem_limit_bytes=LIMIT, **(talk() if jobs else {})),
        cost_estimate=pl.CostEstimate(flops=flops, bytes_accessed=sum(x.size * x.dtype.itemsize for x in args), transcendentals=0),
    )(*args, *ins))
    mine = [got.pop(0) for _ in out_shapes]
    return (*mine, *(job.done([got.pop(0) for _ in job.outs]) for job in jobs))


block = pl.BlockSpec


def columns(size, tile, skip=0):
    return block((size, tile), lambda j: (0, j + skip))


def rows(tile, size):
    return block((tile, size), lambda i: (i, 0))


def once(*size):
    return block(size, lambda *_: (0,) * len(size), pipeline_mode=pl.Buffered(1))


class Sum:
    masks = (CORE, *DIMS, 6, 10, 12)

    def __init__(self, grads, at=(0, 1, 2, 4)):
        self.at, self.ins = at, [*map(cube, grads)]
        self.parts = parts_of(grads)
        self.outs = [shape(*g.shape[4:]) for g in self.ins]
        self.scratch = [VM(g.shape, BF16) for g in self.ins] + chain_scratch(self.ins[0].shape[4], self.parts) + [DMA((len(grads),))]

    def done(self, outs):
        return outs

    def stages(self, ins, outs, scratch):
        held, sem = scratch[: len(ins)], scratch[-1]
        core = bit(CORE)
        mine = lambda: [local(g.at[:, :, :, core], h.at[:, :, :, core], sem, n) for n, (g, h) in enumerate(zip(ins, held))]
        pair, half, quad, end = chain([(ins[n], held[n], outs[n], c) for n, c in self.parts], scratch[len(ins) : -1])

        def loaded():
            wait_all(mine())
            half()

        return [*zip(self.at, (lambda: start_all(mine()), pair, loaded, quad)), (None, end)]


def chain_scratch(rows, parts):
    wide = [c.size for _, c in parts]
    return ([VM((2, 2, 2, rows, w), BF16) for w in wide] + [VM((2, 2, rows, w), BF16) for w in wide] * 2 + [VM((3, rows, w), BF16) for w in wide]
            + [VM((rows, w), F32) for w in wide] + [VM((rows, w), BF16) for w in wide] + [DMA((15,))] * 2 + [DMA((3,))])


def chain(parts, scratch):
    (r, s, t, o, own, res), (send, recv, keep) = [scratch[3 * i : 3 * i + 3] for i in range(6)], scratch[18:]
    core = bit(CORE)

    sems = (send, recv)
    to_core = lambda: [remote(src.at[:, :, :, 1 - core, :, c], r[p], sems, p, CORE) for p, (src, _, _, c) in enumerate(parts)]
    to_next = lambda: [remote(s[p], t[p], sems, 3 + p, DIMS[p]) for p in EACH]
    to_rest = lambda: [c for p in EACH for c in to_three(p, s[p], o[p], sems, 6)]
    keeps = lambda: [local(res[p], out.at[:, c], keep, p) for p, (_, _, out, c) in enumerate(parts)]

    def both(p, place, i, j):
        xyz = [i, j]
        xyz.insert(p, place)
        _, held, _, c = parts[p]
        return held[(*xyz, core, ALL, c)].astype(F32) + r[p][tuple(xyz)].astype(F32)

    def half():
        for c in to_core():
            c.wait_recv()
        for p in EACH:

            def some(n, p=p):
                i, j = n // 2, lax.rem(n, 2)
                s[p][i, j] = both(p, 1 - bit(DIMS[p]), i, j).astype(BF16)

            loop(4, some)
        start_all(to_next())

    def quad():
        for c in to_next():
            c.wait()
        for p in EACH:
            u, v, bu, bv = sides(p)

            def some(n, p=p):
                i, j = n // 2, lax.rem(n, 2)
                s[p][i, j] = (both(p, bit(DIMS[p]), i, j) + t[p][i, j].astype(F32)).astype(BF16)

            own[p][...] = both(p, bit(DIMS[p]), bu, bv) + t[p][bu, bv].astype(F32)
            loop(4, some)
        start_all(to_rest())

    def end():
        for c in to_core():
            c.wait_send()
        wait_all(to_rest())
        for p in EACH:
            res[p][...] = (own[p][...] + sum(o[p][n].astype(F32) for n in EACH)).astype(BF16)
        start_all(keeps())
        wait_all(keeps())

    return lambda: start_all(to_core()), half, quad, end


def unit(h):
    wide = h.astype(F32)
    return wide, lax.rsqrt(jnp.mean(wide * wide, -1, keepdims=True) + 1e-6)


def normed(h):
    wide, scale = unit(h)
    return (wide * scale).astype(BF16)


def unit_back(h, by_normed, by_h):
    wide, scale = unit(h)
    d = by_normed.astype(BF16).astype(F32)
    d = scale * d - wide * (scale * scale * scale * jnp.mean(d * wide, -1, keepdims=True))
    return (by_h.astype(F32) + d.astype(BF16).astype(F32)).astype(BF16)


def turned(t, cos, sin):
    half = t.shape[1] // 2
    a, b = t[:, :half], t[:, half:]
    return jnp.concatenate([a * cos - b * sin, b * cos + a * sin], -1)


def tables(tokens):
    half = HEAD // 2
    angle = jnp.arange(tokens, dtype=F32)[:, None] * THETA ** (-jnp.arange(half, dtype=F32) / half)
    return jnp.cos(angle), jnp.sin(angle)


def head(i):
    return slice(i * HEAD, (i + 1) * HEAD)


def qkv(h, w, cos, sin, jobs=(), tm=256):
    t, d = h.shape
    n = w[0].shape[1]

    def body(h_ref, wq, wk, wv, cos_ref, sin_ref, a_ref, q_ref, k_ref, v_ref):
        a = normed(h_ref[...])
        a_ref[...] = a
        v_ref[...] = nn(a, wv[...]).astype(BF16)
        for w_ref, o_ref in ((wq, q_ref), (wk, k_ref)):
            y = nn(a, w_ref[...]).astype(BF16)
            for i in range(n // HEAD):
                o_ref[:, head(i)] = turned(y[:, head(i)].astype(F32), cos_ref[...], sin_ref[...]).astype(BF16)

    part, angle = rows(tm, n), rows(tm, HEAD // 2)
    return run(body, (t // tm,), [h, *w, cos, sin], [rows(tm, d), *[once(d, n)] * 3, angle, angle], [rows(tm, d), part, part, part],
               [shape(t, d), *[shape(t, n)] * 3], jobs=jobs, flops=6 * t * d * n)


def gap(bk, bq):
    return lax.broadcasted_iota(jnp.int32, (bk, bq), 1) - lax.broadcasted_iota(jnp.int32, (bk, bq), 0)


def blocks_of(iq, bq, bk, one):
    per = bq // bk
    loop(iq * per, lambda j: one(j, None))
    lax.fori_loop(iq * per, iq * per + per, lambda j, _: one(j, j * bk - iq * bq), None)


def attend(q, k, v, jobs=(), bq=512, bk=512, strip=512):
    t, n = q.shape
    scale = HEAD**-0.5
    e = scale * LOG2E
    pieces = [(i, slice(at, at + strip)) for i in range(HEADS) for at in range(0, bq, strip)]

    def body(q_ref, k_ref, v_ref, o_ref, lse_ref, top_s, mix_s):
        top_s[...] = jnp.full(top_s.shape, NEG, F32)
        mix_s[...] = jnp.zeros(mix_s.shape, F32)
        ones = jnp.ones((8, bk), BF16)

        def one(j, hidden):
            here = chunk(j, bk)
            scores = [nt(k_ref[here, head(i)], q_ref[at, head(i)]) for i, at in pieces]
            weights, keeps = [], []
            for (i, at), s in zip(pieces, scores):
                if hidden is not None:
                    s = jnp.where(gap(bk, strip) >= hidden - at.start, s, HIDDEN)
                old = top_s[pl.ds(i, 1), at]
                top = jnp.maximum(old, s.max(axis=0, keepdims=True))
                top_s[pl.ds(i, 1), at] = top
                weights.append(jnp.exp2((s - top) * e).astype(BF16))
                keeps.append(jnp.exp2((old - top) * e))
            for (i, at), p, keep in zip(pieces, weights, keeps):
                values = jnp.concatenate([v_ref[here, head(i)].T, ones], axis=0)
                mix_s[i, :, at] = mix_s[i, :, at] * keep + nn(values, p)

        blocks_of(pl.program_id(0), bq, bk, one)
        for i in range(HEADS):
            total = mix_s[i, HEAD : HEAD + 1, :]
            o_ref[:, head(i)] = (mix_s[i, :HEAD, :] * (1 / total)).T.astype(BF16)
            lse_ref[pl.ds(i, 1), :] = top_s[pl.ds(i, 1), :] * scale + jnp.log(total)

    part = rows(bq, n)
    return run(body, (t // bq,), [q, k, v], [part, once(t, n), once(t, n)], [part, columns(HEADS, bq)],
               [shape(t, n), shape(HEADS, t, dtype=F32)], [VM((HEADS, bq), F32), VM((HEADS, HEAD + 8, bq), F32)],
               jobs=jobs, flops=4 * t * t * n)


def attend_back(q, k, v, out, by_out, lse, cos, sin, jobs=(), bq=512, bk=512, strip=512, together=2):
    t, n = q.shape
    scale = HEAD**-0.5
    e = scale * LOG2E
    width = together * HEAD
    nq = t // bq
    pieces = [(i, slice(at, at + strip)) for i in range(together) for at in range(0, bq, strip)]

    def back(d, cos, sin):
        return turned(d.astype(BF16).astype(F32), cos, -sin).astype(BF16)

    def body(q_ref, k_ref, v_ref, o_ref, do_ref, lse_ref, cos_ref, sin_ref, dq_ref, dk_ref, dv_ref, dq_s, dk_s, dv_s, lse_s, delta_s):
        first, iq = pl.program_id(0) * together, pl.program_id(1)

        @pl.when(iq == 0)
        def _():
            dk_s[...] = jnp.zeros(dk_s.shape, F32)
            dv_s[...] = jnp.zeros(dv_s.shape, F32)

        dq_s[...] = jnp.zeros(dq_s.shape, F32)
        for i in range(together):
            lse_s[pl.ds(i, 1), :] = lse_ref[pl.ds(first + i, 1), :] * LOG2E
            both = do_ref[:, head(i)].astype(F32) * o_ref[:, head(i)].astype(F32)
            delta_s[pl.ds(i, 1), :] = (both[:, : HEAD // 2] + both[:, HEAD // 2 :]).T.sum(axis=0, keepdims=True)

        def one(j, hidden):
            here = chunk(j, bk)
            scores = [nt(k_ref[here, head(i)], q_ref[at, head(i)]) for i, at in pieces]
            dps = [nt(v_ref[here, head(i)], do_ref[at, head(i)]) for i, at in pieces]
            for (i, at), s, dp in zip(pieces, scores, dps):
                p = jnp.exp2(s * e - lse_s[pl.ds(i, 1), at])
                if hidden is not None:
                    p = jnp.where(gap(bk, strip) >= hidden - at.start, p, 0.0)
                ds = (p * (dp - delta_s[pl.ds(i, 1), at])).astype(BF16)
                dv_s[here, head(i)] += nn(p.astype(BF16), do_ref[at, head(i)])
                dk_s[here, head(i)] += nn(ds, q_ref[at, head(i)])
                dq_s[i, :, at] += nn(k_ref[here, head(i)].T, ds)

        blocks_of(iq, bq, bk, one)
        these = chunk(iq, bq)
        for i in range(together):
            dq_ref[:, head(i)] = back((dq_s[i] * scale).T, cos_ref[these, :], sin_ref[these, :])

        @pl.when(iq == nq - 1)
        def _():
            def some(m):
                at = chunk(m, HEAD)
                for i in range(together):
                    dk_ref[at, head(i)] = back(dk_s[at, head(i)] * scale, cos_ref[at, :], sin_ref[at, :])
                dv_ref[at, :] = dv_s[at, :].astype(BF16)

            loop(t // HEAD, some)

    part = block((bq, width), lambda h, i: (i, h))
    whole = block((t, width), lambda h, i: (0, h))
    angle = once(t, HEAD // 2)
    return run(body, (n // width, nq), [q, k, v, out, by_out, lse, cos, sin],
               [part, whole, whole, part, part, block((HEADS, bq), lambda h, i: (0, i)), angle, angle], [part, whole, whole], [shape(t, n)] * 3,
               [VM((together, HEAD, bq), F32), VM((t, width), F32), VM((t, width), F32), VM((8, bq), F32), VM((8, bq), F32)],
               jobs=jobs, flops=10 * t * t * n)


def joined(a, w, h, jobs=(), tm=512, norm=True):
    t, n = h.shape

    def body(a_ref, w_ref, h_ref, o_ref, *b_ref):
        y = nn(a_ref[...], w_ref[...]).astype(BF16)
        new = (h_ref[...].astype(F32) + y.astype(F32)).astype(BF16)
        o_ref[...] = new
        for ref in b_ref:
            ref[...] = normed(new)

    outs = [rows(tm, n)] * (1 + norm)
    return run(body, (t // tm,), [a, w, h], [rows(tm, a.shape[1]), once(*w.shape), rows(tm, n)], outs, [shape(t, n) for _ in outs], jobs=jobs,
               flops=2 * t * n * a.shape[1])


def gated(b, both, jobs=(), tn=512, sub=512):
    t, d = b.shape
    n = both.shape[1] // 2

    def body(b_ref, g_ref, u_ref, act_ref, by_u, by_g):
        for r in range(0, t, sub):
            at = slice(r, r + sub)
            g, u = nn(b_ref[at, :], g_ref[...]), nn(b_ref[at, :], u_ref[...])
            s = jax.nn.sigmoid(g)
            p = g * s
            by_u[at, :] = p
            by_g[at, :] = u * (s + p * (1 - s))
            act_ref[at, :] = (p * u).astype(BF16)

    tile = columns(t, tn)
    return run(body, (n // tn,), [b, both, both], [once(t, d), columns(d, tn), columns(d, tn, n // tn)], [tile] * 3,
               [shape(t, n), shape(t, n, dtype=F32), shape(t, n, dtype=F32)], jobs=jobs, flops=4 * t * d * n)


def gated_back(by_h, down, by_u, by_g, act, jobs=(), tn=256, sub=512):
    t, d = by_h.shape
    n = act.shape[1]

    def body(dh_ref, w_ref, pu_ref, pg_ref, act_ref, dg_ref, du_ref, dw_ref):
        for r in range(0, t, sub):
            at = slice(r, r + sub)
            da = nt(dh_ref[at, :], w_ref[...]).astype(BF16).astype(F32)
            du_ref[at, :] = (da * pu_ref[at, :]).astype(BF16)
            dg_ref[at, :] = (da * pg_ref[at, :]).astype(BF16)
        dw_ref[...] = tt(act_ref[...], dh_ref[...]).astype(BF16)

    tile, w = columns(t, tn), rows(tn, d)
    return run(body, (n // tn,), [by_h, down, by_u, by_g, act], [once(t, d), w, tile, tile, tile], [tile, tile, w],
               [shape(t, n), shape(t, n), shape(n, d)], jobs=jobs, flops=4 * t * d * n)


def mlp_back(by_h, b, h, both, down, by_u, by_g, act, jobs=(), tn=256, sub=512):
    t, d = by_h.shape
    n = act.shape[1]

    def body(dh_ref, b_ref, h_ref, wg_ref, wu_ref, wd_ref, pu_ref, pg_ref, act_ref, dwg_ref, dwu_ref, dwd_ref, o_ref, dg_s, du_s, total):
        j = pl.program_id(0)

        @pl.when(j == 0)
        def _():
            total[...] = jnp.zeros(total.shape, F32)

        for r in range(0, t, sub):
            at = slice(r, r + sub)
            da = nt(dh_ref[at, :], wd_ref[...]).astype(BF16).astype(F32)
            du_s[at, :] = (da * pu_ref[at, :]).astype(BF16)
            dg_s[at, :] = (da * pg_ref[at, :]).astype(BF16)
        dwd_ref[...] = tt(act_ref[...], dh_ref[...]).astype(BF16)
        for r in range(0, t, sub):
            at = slice(r, r + sub)
            total[at, :] += nt(dg_s[at, :], wg_ref[...]) + nt(du_s[at, :], wu_ref[...])
        dwg_ref[...] = tt(b_ref[...], dg_s[...]).astype(BF16)
        dwu_ref[...] = tt(b_ref[...], du_s[...]).astype(BF16)

        @pl.when(j == n // tn - 1)
        def _():
            def some(m):
                at = chunk(m, tn)
                o_ref[at, :] = unit_back(h_ref[at, :], total[at, :], dh_ref[at, :])

            loop(t // tn, some)

    tile, w, wide = columns(t, tn), rows(tn, d), columns(d, tn)
    return run(body, (n // tn,), [by_h, b, h, both, both, down, by_u, by_g, act],
               [once(t, d), once(t, d), once(t, d), wide, columns(d, tn, n // tn), w, tile, tile, tile], [wide, wide, w, block((t, d), lambda j: (0, 0))],
               [shape(d, n), shape(d, n), shape(n, d), shape(t, d)], [VM((t, tn), BF16), VM((t, tn), BF16), VM((t, d), F32)],
               jobs=jobs, flops=12 * t * d * n)


def by_weights(a, ds, jobs=(), tn=512):
    t, m = a.shape
    n = ds[0].shape[1]
    k = len(ds)

    def body(a_ref, *refs):
        for d_ref, o_ref in zip(refs[:k], refs[k:]):
            o_ref[...] = tt(a_ref[...], d_ref[...]).astype(BF16)

    return run(body, (n // tn,), [a, *ds], [once(t, m), *[columns(t, tn)] * k], [columns(m, tn)] * k, [shape(m, n)] * k, jobs=jobs,
               flops=2 * k * t * m * n)


def by_input(ds, ws, h, by_h, jobs=(), tm=256):
    t, n = h.shape
    k = len(ds)

    def body(*refs):
        h_ref, dh_ref, o_ref = refs[2 * k :]
        total = sum(nt(d[...], w[...]) for d, w in zip(refs[:k], refs[k : 2 * k]))
        o_ref[...] = unit_back(h_ref[...], total, dh_ref[...])

    specs = [block((n, d.shape[1]), lambda i, skip=skip: (0, skip), pipeline_mode=pl.Buffered(1)) for d, (_, skip) in zip(ds, ws)]
    return run(body, (t // tm,), [*ds, *[w for w, _ in ws], h, by_h], [*[rows(tm, d.shape[1]) for d in ds], *specs, rows(tm, n), rows(tm, n)], [rows(tm, n)],
               [shape(t, n)], jobs=jobs, flops=sum(2 * t * d.shape[1] * n for d in ds))


def projected_back(by_h, a, w, jobs=(), tn=256):
    t, d = by_h.shape
    n = a.shape[1]

    def body(dh_ref, a_ref, w_ref, da_ref, dw_ref):
        da_ref[...] = nt(dh_ref[...], w_ref[...]).astype(BF16)
        dw_ref[...] = tt(a_ref[...], dh_ref[...]).astype(BF16)

    tile, w_tile = columns(t, tn), rows(tn, d)
    return run(body, (n // tn,), [by_h, a, w], [once(t, d), tile, w_tile], [tile, w_tile], [shape(t, n), shape(n, d)], jobs=jobs,
               flops=4 * t * d * n)


def last_weights(a, ds, jobs=(), tn=512):
    t, m = a.shape
    n = ds[0].shape[1]
    r, k, cut = m // 16, len(ds), n // tn
    steps = k * cut
    masks = Sum.masks
    unit = n // 128
    parts = []
    for turn in range(k):
        wide = [-(-unit // 3)] * 3
        wide[turn] = unit - 2 * wide[turn]
        parts.append([pl.ds(128 * sum(wide[:p]), 128 * wide[p]) for p in EACH])
    sizes = [chain_scratch(r, [(None, c) for c in own]) for own in parts]

    class Chain:
        ins = ()

        def __init__(self):
            self.masks = masks
            self.outs = [shape(r, n)] * k
            self.scratch = [VM((*CUBE, r, n), BF16)] * k + [x for own in sizes for x in own]

        def done(self, outs):
            return outs

        def stages(self, ins, outs, scratch):
            self.held, scratch, self.steps = scratch[:k], scratch[k:], []
            for i in range(k):
                mine = scratch[len(sizes[0]) * i : len(sizes[0]) * (i + 1)]
                self.steps.append(chain([(self.held[i], self.held[i], outs[i], c) for c in parts[i]], mine))
            got = []
            for i, (pair, half, quad, _) in enumerate(self.steps[:-1]):
                at = cut * (i + 1)
                got += [(at, pair), (at + 1, half)] + [(at + 3, quad)] * (at + 3 < steps)
            return [*got, (None, self.rest)]

        def rest(self):
            *_, (_, _, before, _), (pair, half, quad, _) = self.steps
            for what in (pair, before, half, quad, *(s[-1] for s in self.steps)):
                what()

    work = Chain()

    def body(a_ref, *refs):
        j = pl.program_id(0)
        for i in range(k):

            @pl.when(j // cut == i)
            def _(i=i):
                at = chunk(lax.rem(j, cut), tn)
                work.held[i][:, :, :, :, :, at] = tt(a_ref[...], refs[i][...]).astype(BF16).reshape(*CUBE, r, tn)

    specs = [block((t, tn), lambda j, i=i: (0, jnp.clip(j - cut * i, 0, cut - 1))) for i in range(k)]
    return run(body, (steps,), [a, *ds], [once(t, m), *specs], [], [], jobs=[work, *jobs], flops=2 * k * t * m * n)


def join(gradients, sizes):
    pieces = [(i, layer, *p) for i, of in enumerate(gradients) for layer, g in enumerate(of)
              for p in (g if isinstance(g, list) else [(None, pl.ds(0, sizes[i][2]), g)])]
    sums = []
    for _, _, _, _, *arrays in pieces:
        sums += arrays
    others = range(1, 16)
    n = len(sizes)

    def kernel(*refs):
        refs = list(refs)
        take = lambda n: [refs.pop(0) for _ in range(n)]
        s_in, g_out, (total_out,), g_s, r_s = take(len(sums)), take(n), take(1), take(n), take(len(sums))
        acc, tiles, sem, out_sem, send, recv = refs
        hello(others)
        loads = [local(x, r, sem, at) for at, (x, r) in enumerate(zip(s_in, r_s))]
        start_all(loads)
        acc[...] = jnp.zeros(acc.shape, F32)
        at = 0
        for i, layer, _, c, *arrays in pieces:
            mine, at = slice(at, at + len(arrays)), at + len(arrays)
            wait_all(loads[mine])

            def some(m):
                here = chunk(m, 16)
                own, *more = r_s[mine]
                g = own[here, :].astype(F32)
                for x in more:
                    g = g + sum(x[y, here, :].astype(F32) for y in EACH)
                g = g.astype(BF16)
                g_s[i][layer, here, c] = g
                square = g.astype(F32)
                square = square * square
                acc[...] += sum(square[:, 128 * y : 128 * (y + 1)] for y in range(c.size // 128))

            loop(sizes[i][1] // 16, some)
        me = lax.axis_index("dp")
        met(others)

        def copy(m, slot):
            return pltpu.make_async_remote_copy(src_ref=acc, dst_ref=tiles.at[slot], send_sem=send.at[m - 1], recv_sem=recv.at[slot], device_id=peer(m), device_id_type=MESH)

        puts = [local(g, o, out_sem, i) for i, (g, o) in enumerate(zip(g_s, g_out))]
        start_all([*puts, *(copy(m, me) for m in others)])
        tiles[me] = acc[...]
        for m in others:
            copy(m, me).wait_send()
            copy(m, peer(m)["dp"]).wait_recv()
        total = tiles[0]
        for m in others:
            total = total + tiles[m]
        total_out[...] = jnp.broadcast_to(jnp.sum(total, keepdims=True), total.shape)
        wait_all(puts)

    *got, total = pl.pallas_call(
        kernel,
        in_specs=[ANY] * len(sums),
        out_specs=[*[ANY] * n, block(memory_space=VM)],
        out_shape=[*[shape(*z) for z in sizes], shape(16, 128, dtype=F32)],
        scratch_shapes=[*[VM(z, BF16) for z in sizes], *[VM(x.shape, x.dtype) for x in sums], VM((16, 128), F32), VM((16, 16, 128), F32), DMA((len(sums),)),
                        DMA((n,)), DMA((15,)), DMA((16,))],
        compiler_params=pltpu.CompilerParams(vmem_limit_bytes=LIMIT, **talk()),
    )(*sums)
    return got, total


def update(weights, moments, seconds, gradients, total, tiles=8):
    n = len(weights)
    count = 16 * sum(w.size for w in weights)
    flat_all = lambda arrays: [x.reshape(-1, x.shape[-1]) for x in arrays]
    args = [y for x in (weights, moments, seconds, gradients) for y in flat_all(x)]

    def body(total_ref, *refs):
        w_in, m_in, v_in, g_in, w_out, m_out, v_out = (refs[n * i : n * (i + 1)] for i in range(7))
        factor = jnp.minimum(1.0, 0.5 * lax.rsqrt(total_ref[...][:1, :1] / count + 1e-30))
        for i in range(n):
            g, w = g_in[i][...].astype(F32) * factor, w_in[i][...].astype(F32)
            m = 0.9 * m_in[i][...] + 0.1 * g
            v = 0.95 * v_in[i][...] + 0.05 * g * g
            m_out[i][...] = m
            v_out[i][...] = v
            w_out[i][...] = (w - 0.02 * (m * lax.rsqrt(v + 1e-8) + 0.1 * w)).astype(BF16)

    specs = [rows(x.shape[0] // tiles, x.shape[1]) for x in args]
    got = run(body, (tiles,), [total, *args], [once(*total.shape), *specs], specs[: 3 * n], [shape(*x.shape, dtype=x.dtype) for x in args[: 3 * n]])
    return tuple(x.reshape(w.shape) for x, w in zip(got, [*weights] * 3))


def step(x, dy, *arrays):
    wq, wk, wv, wo, gate, up, down = weights = arrays[:7]
    x, dy = x[0], dy[0]
    IDS.clear()
    cos, sin = tables(x.shape[0])
    gathered = lambda w: lax.all_gather(w, "dp", axis=0, tiled=True)
    project = (wq, wk, wv)

    B0 = gathered(jnp.concatenate([gate[0], up[0]], -1))
    Wd0 = gathered(down[0])
    B1 = gathered(jnp.concatenate([gate[1], up[1]], -1))
    Wd1 = gathered(down[1])
    (W0,) = run(None, (1,), [], [], [], [], jobs=[Fetch(project, 0)], flops=10**10)
    a0, q0, k0, v0, (Wo0,) = qkv(x, W0, cos, sin, [Fetch([wo], 0)])
    o0, lse0 = attend(q0, k0, v0)
    h0, b0 = joined(o0, Wo0, x)
    act0, pu0, pg0, W1 = gated(b0, B0, [Fetch(project, 1)])
    (h1,) = joined(act0, Wd0, h0, norm=False)
    a1, q1, k1, v1, (Wo1,) = qkv(h1, W1, cos, sin, [Fetch([wo], 1)])
    o1, lse1 = attend(q1, k1, v1)
    h2, b1 = joined(o1, Wo1, h1)
    act1, pu1, pg1 = gated(b1, B1)

    Dg1, Du1, Dd1, dh2 = mlp_back(dy, b1, h2, B1, Wd1, pu1, pg1, act1)
    do1, Do1, d1p, g1p = projected_back(dh2, o1, Wo1, [Pair([Dd1]), Pair([Dg1])])
    dq1, dk1, dv1, d1h, g1h, u1p, o1p = attend_back(q1, k1, v1, o1, do1, lse1, cos, sin, [Half([Dd1], d1p), Half([Dg1], g1p), Pair([Du1]), Pair([Do1])])
    *D1, d1q = by_weights(a1, [dq1, dk1, dv1], [Quad([Dd1], d1p, d1h)], tn=256)
    dh1, g1q, a1p = by_input([dq1, dk1, dv1], [(w, 0) for w in W1], h1, dh2, [Quad([Dg1], g1p, g1h), Pair(D1)])

    dg0, du0, Dd0, u1h, a1h, o1h = gated_back(dh1, Wd0, pu0, pg0, act0, [Half([Du1], u1p), Half(D1, a1p), Half([Do1], o1p)])
    Dg0, u1q, d0p = by_weights(b0, [dg0], [Quad([Du1], u1p, u1h), Pair([Dd0])])
    Du0, d0h, g0p, o1q = by_weights(b0, [du0], [Half([Dd0], d0p), Pair([Dg0]), Quad([Do1], o1p, o1h)])
    dh0, d0q, g0h, u0p = by_input([dg0, du0], [(B0, 0), (B0, 1)], h0, dh1, [Quad([Dd0], d0p, d0h), Half([Dg0], g0p), Pair([Du0])])
    do0, Do0, a1q = projected_back(dh0, o0, Wo0, [Quad(D1, a1p, a1h)])
    dq0, dk0, dv0, g0q, u0h = attend_back(q0, k0, v0, o0, do0, lse0, cos, sin, [Quad([Dg0], g0p, g0h), Half([Du0], u0p)])
    a0s, u0q, (o0s,) = last_weights(a0, [dq0, dk0, dv0], [Quad([Du0], u0p, u0h), Sum([Do0])])

    of = list(zip([*a0s, o0s, g0q, u0q, d0q], [*split(a1q), o1q, g1q, u1q, d1q]))
    return update(weights, arrays[7:14], arrays[14:21], *join(of, [w.shape for w in weights]))


def split(quad):
    return [[part] for part in quad]


def solution(mesh):
    states, cut = P(("rep", "dp"), None, None), P(None, "dp", None)
    return jax.shard_map(
        step,
        mesh=mesh,
        in_specs=(states, states) + (cut,) * 21,
        out_specs=(P("rep", "dp", None),) * 21,
        check_vma=False,
    )
```

```python
import jax
import jax.numpy as jnp
from jax import lax
from jax.experimental import pallas as pl
from jax.experimental.pallas import tpu as pltpu
from jax.sharding import PartitionSpec as P

F32, BF16 = jnp.float32, jnp.bfloat16
MESH = pl.DeviceIdType.MESH
ANY = pl.BlockSpec(memory_space=pl.ANY)
DMA, VM = pltpu.SemaphoreType.DMA, pltpu.VMEM
LIMIT = 62 * 2**20
WORK = 2 * 10**10
WIDE = 512
HEAD = 256
HEADS = 4
THETA = 10000
LOG2E = 1.4426950408889634
NEG = -1e30
HIDDEN = 2 * NEG
DIMS = (8, 4, 2)
CORE = 1
ALL = slice(None)
EACH = range(3)
CUBE = (2, 2, 2, 2)


def dot(a, b, ca, cb):
    return lax.dot_general(a, b, (((ca,), (cb,)), ((), ())), preferred_element_type=F32)


def nn(a, b):
    return dot(a, b, 1, 0)


def nt(a, b):
    return dot(a, b, 1, 1)


def tt(a, b):
    return dot(a, b, 0, 0)


def shape(*size, dtype=BF16):
    return jax.ShapeDtypeStruct(size, dtype)


def chunk(n, size):
    return pl.ds(pl.multiple_of(n * size, size), size)


def loop(count, what):
    lax.fori_loop(0, count, lambda n, _: what(n), None)


def bit(mask):
    return lax.rem(lax.axis_index("dp") // mask, 2)


def peer(mask):
    at = lax.axis_index("dp")
    for m in (*DIMS, CORE):
        if mask & m:
            at = at + m - 2 * m * bit(m)
    return {"dp": at}


def place():
    return [bit(m) for m in DIMS]


def among(p, at):
    return tuple(at if n == p else ALL for n in EACH)


def parts_of(arrays):
    size = arrays[0].shape[-1]
    if len(arrays) > 1:
        return [(n, pl.ds(0, size)) for n in EACH]
    unit = size // 128
    wide = -(-unit // 3)
    return [(0, pl.ds(128 * wide * n, 128 * min(wide, unit - wide * n))) for n in EACH]


def remote(src, dst, sems, n, mask):
    return pltpu.make_async_remote_copy(src_ref=src, dst_ref=dst, send_sem=sems[0].at[n], recv_sem=sems[1].at[n], device_id=peer(mask), device_id_type=MESH)


def local(src, dst, sems, n):
    return pltpu.make_async_copy(src, dst, sems.at[n])


def start_all(copies):
    for c in copies:
        c.start()


def wait_all(copies):
    for c in copies:
        c.wait()


def flat(ref):
    size = 1
    for n in ref.shape[:-1]:
        size *= n
    return ref.reshape(size, ref.shape[-1])


def added(into, others, size=64):
    into, others = flat(into), [flat(o) for o in others]

    def some(n):
        at = chunk(n, size)
        total = into[at, :].astype(F32)
        for o in others:
            total = total + o[at, :].astype(F32)
        into[at, :] = total.astype(BF16)

    loop(into.shape[0] // size, some)


class Fetch:
    masks = (*DIMS, CORE)

    def __init__(self, ws, layer, at=(1, 3, 5, 7)):
        _, self.rows, self.columns = ws[0].shape
        self.layer, self.at, self.ins, k = layer, at, list(ws), len(ws)
        self.outs = [shape(*CUBE, self.rows, self.columns)] * k
        self.scratch = [VM((k, self.rows, self.columns), BF16), DMA((2 * k,)), DMA((21,)), DMA((21,))]
        self.parts = parts_of(ws)

    def done(self, outs):
        return [o.reshape(16 * self.rows, self.columns) for o in outs]

    def stages(self, ws, fulls, scratch):
        own, sem, *sems = scratch
        b, core, k = place(), bit(CORE), len(ws)
        loads = lambda: [local(w.at[self.layer], own.at[n], sem, n) for n, w in enumerate(ws)]
        keeps = lambda: [local(own.at[n], full.at[(*b, core)], sem, k + n) for n, full in enumerate(fulls)]
        axis = lambda p, level: (p + 2 - level) % 3

        def held(p, level, other=None):
            which, columns = self.parts[p]
            idx = list(b)
            for n in range(level):
                idx[axis(p, n)] = ALL
            if other:
                idx[axis(p, level)] = 1 - b[axis(p, level)]
            return fulls[which].at[(*idx, core, ALL, columns)]

        def first_of(p):
            which, columns = self.parts[p]
            return own.at[which, :, columns]

        def across(p, level):
            return remote(held(p, level) if level else first_of(p), held(p, level), sems, 3 * level + p, DIMS[axis(p, level)])

        def pair(p, level):
            if not level:
                return remote(first_of(p), held(p, level), sems, 9 + p, CORE)
            got = held(p, level - 1, True)
            return remote(got, got, sems, 9 + 3 * level + p, CORE)

        def begin():
            start_all(loads())

        def first():
            wait_all(loads())
            start_all(keeps())
            start_all([across(p, 0) for p in EACH] + [pair(p, 0) for p in EACH])

        def next_of(level):
            def go():
                if level == 1:
                    wait_all(keeps())
                for p in EACH:
                    across(p, level - 1).wait_recv()
                    if level < 3:
                        across(p, level).start()
                    pair(p, level).start()

            return go

        def end():
            for p in EACH:
                for level in EACH:
                    across(p, level).wait_send()
                wait_all([pair(p, level) for level in range(4)])

        return [(0, begin), *zip(self.at, (first, *(next_of(n + 1) for n in EACH))), (None, end)]


def cube(g):
    return g if len(g.shape) > len(CUBE) else g.reshape(*CUBE, g.shape[0] // 16, g.shape[1])


class Mine:
    def __init__(self, index, *size):
        self.index, self.shape = index, size


def given(arrays):
    return [x for x in arrays if not isinstance(x, Mine)] if isinstance(arrays, list) else []


def gradients_of(job, refs):
    n = len(given(job.grads))
    return refs[:n] or [job.outer[g.index] for g in job.grads], refs[n:]


class Pair:
    masks = (CORE,)
    followed = None

    def __init__(self, grads, at=1):
        self.grads = [cube(g) for g in grads]
        self.at, self.ins = at, given(self.grads)
        self.outs = [shape(*CUBE[1:], *g.shape[4:]) for g in self.grads]
        self.scratch = [DMA((len(grads),))] * 2

    def done(self, outs):
        return outs

    def stages(self, ins, outs, sems):
        self.refs = outs
        grads, _ = gradients_of(self, ins)
        self.copies = lambda: [remote(g.at[:, :, :, 1 - bit(CORE)], r, sems, n, CORE) for n, (g, r) in enumerate(zip(grads, outs))]
        return [(self.at, lambda: start_all(self.copies())), (None, lambda: left(self))]


def left(job):
    for c in job.copies():
        if job.followed:
            c.wait_send()
        else:
            c.wait()


def follow(before, refs):
    if isinstance(before, list):
        return refs, lambda: None
    before.followed = True

    def arrive():
        for c in before.copies():
            c.wait_recv()

    return before.refs, arrive


class Half:
    masks = DIMS
    followed = None

    def __init__(self, grads, pairs, at=(0, 1, 1)):
        self.at, self.grads, self.parts, self.pairs = at, [*map(cube, grads)], parts_of(grads), pairs
        self.ins = [*given(self.grads), *given(pairs)]
        self.sizes = [(2, 2, self.grads[0].shape[4], c.size) for _, c in self.parts]
        self.outs = [shape(*s) for s in self.sizes]
        self.scratch = [VM(s, BF16) for s in self.sizes] * 2 + [DMA((6,)), DMA((3,)), DMA((3,))]

    def done(self, outs):
        return outs

    def stages(self, ins, outs, scratch):
        grads, ins = gradients_of(self, ins)
        pairs, arrive = follow(self.pairs, ins)
        a, r, (sem, *sems) = scratch[:3], scratch[3:6], scratch[6:]
        self.refs, self.spare = outs, r

        def loads():
            got = []
            for p, (n, columns) in enumerate(self.parts):
                at = among(p, 1 - bit(DIMS[p]))
                got.append(local(grads[n].at[(*at, bit(CORE), ALL, columns)], a[p], sem, p))
                got.append(local(pairs[n].at[(*at, ALL, columns)], r[p], sem, 3 + p))
            return got

        def begin():
            arrive()
            start_all(loads())

        def add():
            wait_all(loads())
            for p in EACH:
                added(a[p], [r[p]])

        self.copies = lambda: [remote(a[p], outs[p], sems, p, DIMS[p]) for p in EACH]
        return [*zip(self.at, (begin, add, lambda: start_all(self.copies()))), (None, lambda: left(self))]


class Quad:
    masks = (2, 4, 6, 8, 10, 12)

    def __init__(self, grads, pairs, halves, at=(0, 1, 1)):
        self.at, self.grads, self.parts, self.pairs, self.halves = at, [*map(cube, grads)], parts_of(grads), pairs, halves
        self.ins = [*given(self.grads), *given(pairs), *given(halves)]
        rows = self.grads[0].shape[4]
        self.outs = [shape(rows, c.size, dtype=F32) for _, c in self.parts] + [shape(3, rows, c.size) for _, c in self.parts]
        self.scratch = [VM((2, 2, rows, c.size), BF16) for _, c in self.parts] * (3 if given(halves) else 2) + [VM((rows, c.size), F32) for _, c in self.parts]
        self.scratch += [DMA((12,)), DMA((9,)), DMA((9,))]

    def done(self, outs):
        return [(*part, *sums) for part, *sums in zip(self.parts, outs[:3], outs[3:])]

    def stages(self, ins, outs, scratch):
        grads, ins = gradients_of(self, ins)
        m = len(given(self.pairs))
        pairs, _ = follow(self.pairs, ins[:m])
        halves, arrive = follow(self.halves, ins[m:])
        sem, *sems = scratch[-3:]
        a, s, own, r = scratch[:3], scratch[3:6], scratch[-6:-3], getattr(self.halves, "spare", scratch[6:9])

        def loads():
            got = []
            for p, (n, columns) in enumerate(self.parts):
                at = among(p, bit(DIMS[p]))
                got.append(local(grads[n].at[(*at, bit(CORE), ALL, columns)], a[p], sem, p))
                got.append(local(pairs[n].at[(*at, ALL, columns)], r[p], sem, 3 + p))
                got.append(local(halves[p], s[p], sem, 6 + p))
            return got

        def begin():
            arrive()
            start_all(loads())

        def add():
            wait_all(loads())
            for p in EACH:
                total_of(p, own[p], a[p], r[p], s[p])
                added(a[p], [r[p], s[p]])

        copies = lambda: [local(own[p], outs[p], sem, 9 + p) for p in EACH] + [c for p in EACH for c in to_three(p, a[p], outs[3 + p], sems)]
        return [*zip(self.at, (begin, add, lambda: start_all(copies()))), (None, lambda: wait_all(copies()))]


def chained(grads, ready=0, third=4):
    pair = Pair(grads, ready + 1)
    half = Half(grads, pair, at_once(ready + 3))
    return [pair, half, Quad(grads, pair, half, at_once(ready + 3 + third))]


def at_once(n):
    return n, n + 1, n + 1


def sides(p):
    u, v = (n for n in EACH if n != p)
    return u, v, bit(DIMS[u]), bit(DIMS[v])


def total_of(p, own, *terms, size=64):
    _, _, bu, bv = sides(p)

    def some(n):
        at = chunk(n, size)
        own[at, :] = sum(x[bu, bv, at, :].astype(F32) for x in terms)

    loop(own.shape[0] // size, some)


def to_three(p, blocks, others, sems, base=0):
    u, v, bu, bv = sides(p)
    flips = ((1, 0), (0, 1), (1, 1))
    return [remote(blocks.at[1 - bu if fu else bu, 1 - bv if fv else bv], others.at[n], sems, base + 3 * p + n, DIMS[u] * fu + DIMS[v] * fv)
            for n, (fu, fv) in enumerate(flips)]


IDS = []


def talk():
    IDS.append(None)
    return dict(collective_id=len(IDS), has_side_effects=True)


def hello(masks):
    for m in masks:
        pl.semaphore_signal(pltpu.get_barrier_semaphore(), inc=1, device_id=peer(m), device_id_type=MESH)


def met(masks):
    pl.semaphore_wait(pltpu.get_barrier_semaphore(), len(masks))


def run(body, grid, args, in_specs, out_specs, out_shapes, scratch=(), jobs=()):
    steps = 1
    for g in grid:
        steps *= g
    gather = lambda name: [x for job in jobs for x in getattr(job, name)]
    ins, outs, scr = gather("ins"), gather("outs"), gather("scratch")
    masks = sorted(set(gather("masks")))

    def kernel(*refs):
        refs = list(refs)
        take = lambda held, n: [held.pop(0) for _ in range(n)]
        my_in, job_in, my_out, job_out, my_scr, job_scr = (take(refs, len(x)) for x in (args, ins, out_shapes, outs, scratch, scr))
        step = 0
        for axis, g in enumerate(grid):
            step = step * g + pl.program_id(axis)
        plan = {}
        for job in jobs:
            job.outer = my_out
            for at, what in job.stages(take(job_in, len(job.ins)), take(job_out, len(job.outs)), take(job_scr, len(job.scratch))):
                plan.setdefault(at if at is None else min(at, steps - 1), []).append(what)
        last = plan.pop(None, [])
        if jobs:
            plan.setdefault(0, []).insert(0, lambda: hello(masks))
            greet = min(1, steps - 1)
            plan.setdefault(greet, []).insert(1 - greet, lambda: met(masks))
        for at in sorted(plan):

            @pl.when(step == at)
            def _(todo=plan[at]):
                for what in todo:
                    what()

        if body is not None:
            body(*my_in, *my_out, *my_scr)
        if last:

            @pl.when(step == steps - 1)
            def _():
                for what in last:
                    what()

    got = list(pl.pallas_call(
        kernel,
        grid=grid,
        in_specs=[*in_specs, *[ANY] * len(ins)],
        out_specs=[*out_specs, *[ANY] * len(outs)],
        out_shape=[*out_shapes, *outs],
        scratch_shapes=[*scratch, *scr],
        compiler_params=pltpu.CompilerParams(dimension_semantics=("arbitrary",) * len(grid), vmem_limit_bytes=LIMIT, **(talk() if jobs else {})),
        cost_estimate=pl.CostEstimate(flops=WORK, bytes_accessed=sum(x.size * x.dtype.itemsize for x in args), transcendentals=0),
    )(*args, *ins))
    mine = [got.pop(0) for _ in out_shapes]
    return (*mine, *(job.done([got.pop(0) for _ in job.outs]) for job in jobs))


block = pl.BlockSpec


def columns(size, tile, skip=0):
    return block((size, tile), lambda j: (0, j + skip))


def slices(size, tile):
    return [slice(n, n + tile) for n in range(0, size, tile)]


def rows(tile, size):
    return block((tile, size), lambda i: (i, 0))


def once(*size):
    return block(size, lambda *_: (0,) * len(size), pipeline_mode=pl.Buffered(1))


class Sum:
    masks = (CORE, *DIMS, 6, 10, 12)

    def __init__(self, grads, at=(0, 1, 2, 4)):
        self.at, self.ins = at, [*map(cube, grads)]
        self.parts = parts_of(grads)
        self.outs = [shape(*g.shape[4:]) for g in self.ins]
        self.scratch = [VM(g.shape, BF16) for g in self.ins] + chain_scratch(self.ins[0].shape[4], self.parts) + [DMA((len(grads),))]

    def done(self, outs):
        return outs

    def stages(self, ins, outs, scratch):
        held, sem = scratch[: len(ins)], scratch[-1]
        core = bit(CORE)
        mine = lambda: [local(g.at[:, :, :, core], h.at[:, :, :, core], sem, n) for n, (g, h) in enumerate(zip(ins, held))]
        pair, half, quad, end = chain([(ins[n], held[n], outs[n], c) for n, c in self.parts], scratch[len(ins) : -1])

        def loaded():
            wait_all(mine())
            half()

        return [*zip(self.at, (lambda: start_all(mine()), pair, loaded, quad)), (None, end)]


def chain_scratch(rows, parts):
    wide = [c.size for _, c in parts]
    return ([VM((2, 2, 2, rows, w), BF16) for w in wide] + [VM((2, 2, rows, w), BF16) for w in wide] * 2 + [VM((3, rows, w), BF16) for w in wide]
            + [VM((rows, w), F32) for w in wide] + [VM((rows, w), BF16) for w in wide] + [DMA((15,))] * 2 + [DMA((3,))])


def chain(parts, scratch):
    (r, s, t, o, own, res), (send, recv, keep) = [scratch[3 * i : 3 * i + 3] for i in range(6)], scratch[18:]
    core = bit(CORE)

    sems = (send, recv)
    to_core = lambda: [remote(src.at[:, :, :, 1 - core, :, c], r[p], sems, p, CORE) for p, (src, _, _, c) in enumerate(parts)]
    to_next = lambda: [remote(s[p], t[p], sems, 3 + p, DIMS[p]) for p in EACH]
    to_rest = lambda: [c for p in EACH for c in to_three(p, s[p], o[p], sems, 6)]
    keeps = lambda: [local(res[p], out.at[:, c], keep, p) for p, (_, _, out, c) in enumerate(parts)]

    def both(p, place, i, j):
        xyz = [i, j]
        xyz.insert(p, place)
        _, held, _, c = parts[p]
        return held[(*xyz, core, ALL, c)].astype(F32) + r[p][tuple(xyz)].astype(F32)

    def half():
        for c in to_core():
            c.wait_recv()
        for p in EACH:

            def some(n, p=p):
                i, j = n // 2, lax.rem(n, 2)
                s[p][i, j] = both(p, 1 - bit(DIMS[p]), i, j).astype(BF16)

            loop(4, some)
        start_all(to_next())

    def quad():
        for c in to_next():
            c.wait()
        for p in EACH:
            u, v, bu, bv = sides(p)

            def some(n, p=p):
                i, j = n // 2, lax.rem(n, 2)
                s[p][i, j] = (both(p, bit(DIMS[p]), i, j) + t[p][i, j].astype(F32)).astype(BF16)

            own[p][...] = both(p, bit(DIMS[p]), bu, bv) + t[p][bu, bv].astype(F32)
            loop(4, some)
        start_all(to_rest())

    def end():
        for c in to_core():
            c.wait_send()
        wait_all(to_rest())
        for p in EACH:
            res[p][...] = (own[p][...] + sum(o[p][n].astype(F32) for n in EACH)).astype(BF16)
        start_all(keeps())
        wait_all(keeps())

    return lambda: start_all(to_core()), half, quad, end


def unit(h):
    wide = h.astype(F32)
    return wide, lax.rsqrt(jnp.mean(wide * wide, -1, keepdims=True) + 1e-6)


def normed(h):
    wide, scale = unit(h)
    return (wide * scale).astype(BF16)


def unit_back(h, by_normed, by_h):
    wide, scale = unit(h)
    d = by_normed.astype(BF16).astype(F32)
    d = scale * d - wide * (scale * scale * scale * jnp.mean(d * wide, -1, keepdims=True))
    return (by_h.astype(F32) + d.astype(BF16).astype(F32)).astype(BF16)


def turned(t, cos, sin):
    half = t.shape[1] // 2
    a, b = t[:, :half], t[:, half:]
    return jnp.concatenate([a * cos - b * sin, b * cos + a * sin], -1)


def tables(tokens):
    half = HEAD // 2
    angle = jnp.arange(tokens, dtype=F32)[:, None] * THETA ** (-jnp.arange(half, dtype=F32) / half)
    return jnp.cos(angle), jnp.sin(angle)


def head(i):
    return slice(i * HEAD, (i + 1) * HEAD)


def qkv(h, w, cos, sin, jobs=(), tm=HEAD):
    t, d = h.shape
    n = w[0].shape[1]

    def body(h_ref, wq, wk, wv, cos_ref, sin_ref, a_ref, q_ref, k_ref, v_ref):
        a = normed(h_ref[...])
        a_ref[...] = a
        v_ref[...] = nn(a, wv[...]).astype(BF16)
        for w_ref, o_ref in ((wq, q_ref), (wk, k_ref)):
            y = nn(a, w_ref[...]).astype(BF16)
            for i in range(n // HEAD):
                o_ref[:, head(i)] = turned(y[:, head(i)].astype(F32), cos_ref[...], sin_ref[...]).astype(BF16)

    part, angle = rows(tm, n), rows(tm, HEAD // 2)
    return run(body, (t // tm,), [h, *w, cos, sin], [rows(tm, d), *[once(d, n)] * 3, angle, angle], [rows(tm, d), part, part, part],
               [shape(t, d), *[shape(t, n)] * 3], jobs=jobs)


def gap(bk, bq):
    return lax.broadcasted_iota(jnp.int32, (bk, bq), 1) - lax.broadcasted_iota(jnp.int32, (bk, bq), 0)


def blocks_of(iq, bq, bk, one):
    per = bq // bk
    loop(iq * per, lambda j: one(j, None))
    lax.fori_loop(iq * per, iq * per + per, lambda j, _: one(j, j * bk - iq * bq), None)


def attend(q, k, v, jobs=(), bq=WIDE, bk=WIDE, strip=WIDE):
    t, n = q.shape
    scale = HEAD**-0.5
    e = scale * LOG2E
    pieces = [(i, at) for i in range(HEADS) for at in slices(bq, strip)]

    def body(q_ref, k_ref, v_ref, o_ref, lse_ref, top_s, mix_s):
        top_s[...] = jnp.full(top_s.shape, NEG, F32)
        mix_s[...] = jnp.zeros(mix_s.shape, F32)
        ones = jnp.ones((8, bk), BF16)

        def one(j, hidden):
            here = chunk(j, bk)
            scores = [nt(k_ref[here, head(i)], q_ref[at, head(i)]) for i, at in pieces]
            weights, keeps = [], []
            for (i, at), s in zip(pieces, scores):
                if hidden is not None:
                    s = jnp.where(gap(bk, strip) >= hidden - at.start, s, HIDDEN)
                old = top_s[pl.ds(i, 1), at]
                top = jnp.maximum(old, s.max(axis=0, keepdims=True))
                top_s[pl.ds(i, 1), at] = top
                weights.append(jnp.exp2((s - top) * e).astype(BF16))
                keeps.append(jnp.exp2((old - top) * e))
            for (i, at), p, keep in zip(pieces, weights, keeps):
                values = jnp.concatenate([v_ref[here, head(i)].T, ones], axis=0)
                mix_s[i, :, at] = mix_s[i, :, at] * keep + nn(values, p)

        blocks_of(pl.program_id(0), bq, bk, one)
        for i in range(HEADS):
            total = mix_s[i, HEAD : HEAD + 1, :]
            o_ref[:, head(i)] = (mix_s[i, :HEAD, :] * (1 / total)).T.astype(BF16)
            lse_ref[pl.ds(i, 1), :] = top_s[pl.ds(i, 1), :] * scale + jnp.log(total)

    part = rows(bq, n)
    return run(body, (t // bq,), [q, k, v], [part, once(t, n), once(t, n)], [part, columns(HEADS, bq)],
               [shape(t, n), shape(HEADS, t, dtype=F32)], [VM((HEADS, bq), F32), VM((HEADS, HEAD + 8, bq), F32)],
               jobs=jobs)


def attend_back(q, k, v, out, by_out, lse, cos, sin, jobs=(), bq=WIDE, bk=WIDE, strip=WIDE, together=2):
    t, n = q.shape
    scale = HEAD**-0.5
    e = scale * LOG2E
    width = together * HEAD
    nq = t // bq
    pieces = [(i, at) for i in range(together) for at in slices(bq, strip)]

    def back(d, cos, sin):
        return turned(d.astype(BF16).astype(F32), cos, -sin).astype(BF16)

    def body(q_ref, k_ref, v_ref, o_ref, do_ref, lse_ref, cos_ref, sin_ref, dq_ref, dk_ref, dv_ref, dq_s, dk_s, dv_s, lse_s, delta_s):
        first, iq = pl.program_id(0) * together, pl.program_id(1)

        @pl.when(iq == 0)
        def _():
            dk_s[...] = jnp.zeros(dk_s.shape, F32)
            dv_s[...] = jnp.zeros(dv_s.shape, F32)

        dq_s[...] = jnp.zeros(dq_s.shape, F32)
        for i in range(together):
            lse_s[pl.ds(i, 1), :] = lse_ref[pl.ds(first + i, 1), :] * LOG2E
            both = do_ref[:, head(i)].astype(F32) * o_ref[:, head(i)].astype(F32)
            delta_s[pl.ds(i, 1), :] = (both[:, : HEAD // 2] + both[:, HEAD // 2 :]).T.sum(axis=0, keepdims=True)

        def one(j, hidden):
            here = chunk(j, bk)
            scores = [nt(k_ref[here, head(i)], q_ref[at, head(i)]) for i, at in pieces]
            dps = [nt(v_ref[here, head(i)], do_ref[at, head(i)]) for i, at in pieces]
            for (i, at), s, dp in zip(pieces, scores, dps):
                p = jnp.exp2(s * e - lse_s[pl.ds(i, 1), at])
                if hidden is not None:
                    p = jnp.where(gap(bk, strip) >= hidden - at.start, p, 0.0)
                ds = (p * (dp - delta_s[pl.ds(i, 1), at])).astype(BF16)
                dv_s[here, head(i)] += nn(p.astype(BF16), do_ref[at, head(i)])
                dk_s[here, head(i)] += nn(ds, q_ref[at, head(i)])
                dq_s[i, :, at] += nn(k_ref[here, head(i)].T, ds)

        blocks_of(iq, bq, bk, one)
        these = chunk(iq, bq)
        for i in range(together):
            dq_ref[:, head(i)] = back((dq_s[i] * scale).T, cos_ref[these, :], sin_ref[these, :])

        @pl.when(iq == nq - 1)
        def _():
            def some(m):
                at = chunk(m, HEAD)
                for i in range(together):
                    dk_ref[at, head(i)] = back(dk_s[at, head(i)] * scale, cos_ref[at, :], sin_ref[at, :])
                dv_ref[at, :] = dv_s[at, :].astype(BF16)

            loop(t // HEAD, some)

    part = block((bq, width), lambda h, i: (i, h))
    whole = block((t, width), lambda h, i: (0, h))
    angle = once(t, HEAD // 2)
    return run(body, (n // width, nq), [q, k, v, out, by_out, lse, cos, sin],
               [part, whole, whole, part, part, block((HEADS, bq), lambda h, i: (0, i)), angle, angle], [part, whole, whole], [shape(t, n)] * 3,
               [VM((together, HEAD, bq), F32), VM((t, width), F32), VM((t, width), F32), VM((8, bq), F32), VM((8, bq), F32)],
               jobs=jobs)


def joined(a, w, h, jobs=(), tm=WIDE, norm=True, skip=0):
    t, n = h.shape

    def body(a_ref, w_ref, h_ref, o_ref, *b_ref):
        y = nn(a_ref[...], w_ref[...]).astype(BF16)
        new = (h_ref[...].astype(F32) + y.astype(F32)).astype(BF16)
        o_ref[...] = new
        for ref in b_ref:
            ref[...] = normed(new)

    outs = [rows(tm, n)] * (1 + norm)
    return run(body, (t // tm,), [a, w, h], [rows(tm, a.shape[1]), block((a.shape[1], n), lambda i: (0, skip), pipeline_mode=pl.Buffered(1)), rows(tm, n)], outs, [shape(t, n) for _ in outs], jobs=jobs)


def gated(b, both, n, jobs=(), tn=WIDE, sub=WIDE):
    t, d = b.shape

    def body(b_ref, g_ref, u_ref, act_ref, by_u, by_g):
        for at in slices(t, sub):
            g, u = nn(b_ref[at, :], g_ref[...]), nn(b_ref[at, :], u_ref[...])
            s = jax.nn.sigmoid(g)
            p = g * s
            by_u[at, :] = p
            by_g[at, :] = u * (s + p * (1 - s))
            act_ref[at, :] = (p * u).astype(BF16)

    tile = columns(t, tn)
    return run(body, (n // tn,), [b, both, both], [once(t, d), columns(d, tn), columns(d, tn, n // tn)], [tile] * 3,
               [shape(t, n), shape(t, n, dtype=F32), shape(t, n, dtype=F32)], jobs=jobs)


def mlp_back(by_h, b, both, down, by_u, by_g, h, jobs, cut, tn=HEAD, sub=WIDE):
    t, d = by_h.shape
    n = by_u.shape[1]
    tiles = n // tn
    sizes = [(*CUBE, d // 16, tn * k) for k in (cut, cut, tiles - cut, tiles - cut)]

    def body(dh_ref, b_ref, wg_ref, wu_ref, wd_ref, pu_ref, pg_ref, h_ref, *refs):
        *outs, out, dg_s, du_s, total, mine, up_s, gate_s, sem = refs
        staged = gate_s, up_s
        j = pl.program_id(0)

        def stores(outs, skip):
            return [local(x, o.at[(*[ALL] * 5, chunk(j - skip, tn))], sem, i) for i, (x, o) in enumerate(zip(staged, outs))]

        @pl.when(j == 0)
        def _():
            total[...] = jnp.zeros(total.shape, F32)

        cuts = slices(t, sub)
        for at in cuts:
            da = nt(dh_ref[at, :], wd_ref[...]).astype(BF16).astype(F32)
            du_s[at, :] = (da * pu_ref[at, :]).astype(BF16)
            dg_s[at, :] = (da * pg_ref[at, :]).astype(BF16)
        for at in cuts:
            total[at, :] += nt(dg_s[at, :], wg_ref[...]) + nt(du_s[at, :], wu_ref[...])

        @pl.when(j > 0)
        def _():
            wait_all(stores(outs, j))

        for x, s in zip((dg_s, du_s), staged):
            s[...] = tt(b_ref[...], x[...]).astype(BF16).reshape(s.shape)

        @pl.when(j < cut)
        def _():
            start_all(stores(outs, 0))

        @pl.when(j >= cut)
        def _():
            start_all(stores(outs[2:], cut))

        @pl.when(j == tiles - 1)
        def _():
            def some(m):
                at = chunk(m, tn)
                mine[at, :] = unit_back(h_ref[at, :], total[at, :], dh_ref[at, :])

            loop(t // tn, some)
            last = [local(mine, out, sem, len(outs)), *stores(outs, j)]
            last[0].start()
            wait_all(last)

    tile = columns(t, tn)
    whole = once(t, d)
    return run(body, (tiles,), [by_h, b, both, both, down, by_u, by_g, h],
               [whole, whole, columns(d, tn), columns(d, tn, tiles), rows(tn, d), tile, tile, whole], [ANY] * 5,
               [*[shape(*s) for s in sizes], shape(t, d)],
               [VM((t, tn), BF16), VM((t, tn), BF16), VM((t, d), F32), VM((t, d), BF16), *[VM((*CUBE, d // 16, tn), BF16)] * 2, DMA((5,))],
               jobs=[*jobs, *(c for i in (0, 1) for c in chained([Mine(i, *sizes[i])], cut))])


def by_weight(a, d, jobs=(), tm=WIDE):
    t, m = a.shape
    n = d.shape[1]

    def body(a_ref, d_ref, o_ref):
        o_ref[...] = tt(a_ref[...], d_ref[...]).astype(BF16)

    return run(body, (m // tm,), [a, d], [columns(t, tm), once(t, n)], [rows(tm, n)], [shape(m, n)], jobs=jobs)


def by_weights(a, ds, jobs=(), tn=WIDE):
    t, m = a.shape
    n = ds[0].shape[1]
    k = len(ds)

    def body(a_ref, *refs):
        for d_ref, o_ref in zip(refs[:k], refs[k:]):
            o_ref[...] = tt(a_ref[...], d_ref[...]).astype(BF16)

    return run(body, (n // tn,), [a, *ds], [once(t, m), *[columns(t, tn)] * k], [columns(m, tn)] * k, [shape(m, n)] * k, jobs=jobs)


def by_input(ds, ws, h, by_h, jobs=(), tm=HEAD):
    t, n = h.shape
    k = len(ds)

    def body(*refs):
        h_ref, dh_ref, o_ref = refs[2 * k :]
        total = sum(nt(d[...], w[...]) for d, w in zip(refs[:k], refs[k : 2 * k]))
        o_ref[...] = unit_back(h_ref[...], total, dh_ref[...])

    specs = [block((n, d.shape[1]), lambda i, skip=skip: (0, skip), pipeline_mode=pl.Buffered(1)) for d, (_, skip) in zip(ds, ws)]
    return run(body, (t // tm,), [*ds, *[w for w, _ in ws], h, by_h], [*[rows(tm, d.shape[1]) for d in ds], *specs, rows(tm, n), rows(tm, n)], [rows(tm, n)],
               [shape(t, n)], jobs=jobs)


def projected_back(by_h, a, w, skip, jobs=(), tn=HEAD):
    t, d = by_h.shape
    n = a.shape[1]

    def body(dh_ref, a_ref, w_ref, da_ref, dw_ref):
        da_ref[...] = nt(dh_ref[...], w_ref[...]).astype(BF16)
        dw_ref[...] = tt(a_ref[...], dh_ref[...]).astype(BF16)

    tile = columns(t, tn)
    return run(body, (n // tn,), [by_h, a, w], [once(t, d), tile, block((tn, d), lambda j: (j, skip))], [tile, rows(tn, d)], [shape(t, n), shape(n, d)], jobs=jobs)


def last_weights(a, ds, jobs=(), tn=WIDE):
    t, m = a.shape
    n = ds[0].shape[1]
    r, k, cut = m // 16, len(ds), n // tn
    steps = k * cut
    masks = Sum.masks
    unit = n // 128
    parts = []
    for turn in range(k):
        wide = [-(-unit // 3)] * 3
        wide[turn] = unit - 2 * wide[turn]
        parts.append([pl.ds(128 * sum(wide[:p]), 128 * wide[p]) for p in EACH])
    sizes = [chain_scratch(r, [(None, c) for c in own]) for own in parts]

    class Chain:
        ins = ()

        def __init__(self):
            self.masks = masks
            self.outs = [shape(r, n)] * k
            self.scratch = [VM((*CUBE, r, n), BF16)] * k + [x for own in sizes for x in own]

        def done(self, outs):
            return outs

        def stages(self, ins, outs, scratch):
            self.held, scratch, self.steps = scratch[:k], scratch[k:], []
            for i in range(k):
                mine = scratch[len(sizes[0]) * i : len(sizes[0]) * (i + 1)]
                self.steps.append(chain([(self.held[i], self.held[i], outs[i], c) for c in parts[i]], mine))
            got = []
            for i, (pair, half, quad, _) in enumerate(self.steps[:-1]):
                at = cut * (i + 1)
                got += [(at, pair), (at + 1, half)] + [(at + 3, quad)] * (at + 3 < steps)
            return [*got, (None, self.rest)]

        def rest(self):
            *_, (_, _, before, _), (pair, half, quad, _) = self.steps
            for what in (pair, before, half, quad, *(s[-1] for s in self.steps)):
                what()

    work = Chain()

    def body(a_ref, *refs):
        j = pl.program_id(0)
        for i in range(k):

            @pl.when(j // cut == i)
            def _(i=i):
                at = chunk(lax.rem(j, cut), tn)
                work.held[i][:, :, :, :, :, at] = tt(a_ref[...], refs[i][...]).astype(BF16).reshape(*CUBE, r, tn)

    specs = [block((t, tn), lambda j, i=i: (0, jnp.clip(j - cut * i, 0, cut - 1))) for i in range(k)]
    return run(body, (steps,), [a, *ds], [once(t, m), *specs], [], [], jobs=[work, *jobs])


def join(gradients, sizes):
    pieces = [(i, layer, *p) for i, of in enumerate(gradients) for layer, g in enumerate(of)
              for p in (g if isinstance(g, list) else [(None, pl.ds(0, sizes[i][2]), g)])]
    sums = []
    for _, _, _, _, *arrays in pieces:
        sums += arrays
    others = range(1, 16)
    n = len(sizes)

    def kernel(*refs):
        refs = list(refs)
        take = lambda n: [refs.pop(0) for _ in range(n)]
        s_in, g_out, (total_out,), g_s, r_s = take(len(sums)), take(n), take(1), take(n), take(len(sums))
        acc, tiles, sem, out_sem, send, recv = refs
        hello(others)
        loads = [local(x, r, sem, at) for at, (x, r) in enumerate(zip(s_in, r_s))]
        start_all(loads)
        acc[...] = jnp.zeros(acc.shape, F32)
        at = 0
        for i, layer, _, c, *arrays in pieces:
            mine, at = slice(at, at + len(arrays)), at + len(arrays)
            wait_all(loads[mine])

            def some(m):
                here = chunk(m, 16)
                own, *more = r_s[mine]
                g = own[here, :].astype(F32)
                for x in more:
                    g = g + sum(x[y, here, :].astype(F32) for y in EACH)
                g = g.astype(BF16)
                g_s[i][layer, here, c] = g
                square = g.astype(F32)
                square = square * square
                acc[...] += sum(square[:, 128 * y : 128 * (y + 1)] for y in range(c.size // 128))

            loop(sizes[i][1] // 16, some)
        me = lax.axis_index("dp")
        met(others)

        def copy(m, slot):
            return pltpu.make_async_remote_copy(src_ref=acc, dst_ref=tiles.at[slot], send_sem=send.at[m - 1], recv_sem=recv.at[slot], device_id=peer(m), device_id_type=MESH)

        puts = [local(g, o, out_sem, i) for i, (g, o) in enumerate(zip(g_s, g_out))]
        start_all([*puts, *(copy(m, me) for m in others)])
        tiles[me] = acc[...]
        for m in others:
            copy(m, me).wait_send()
            copy(m, peer(m)["dp"]).wait_recv()
        total = tiles[0]
        for m in others:
            total = total + tiles[m]
        total_out[...] = jnp.broadcast_to(jnp.sum(total, keepdims=True), total.shape)
        wait_all(puts)

    *got, total = pl.pallas_call(
        kernel,
        in_specs=[ANY] * len(sums),
        out_specs=[*[ANY] * n, block(memory_space=VM)],
        out_shape=[*[shape(*z) for z in sizes], shape(16, 128, dtype=F32)],
        scratch_shapes=[*[VM(z, BF16) for z in sizes], *[VM(x.shape, x.dtype) for x in sums], VM((16, 128), F32), VM((16, 16, 128), F32), DMA((len(sums),)),
                        DMA((n,)), DMA((15,)), DMA((16,))],
        compiler_params=pltpu.CompilerParams(vmem_limit_bytes=LIMIT, **talk()),
    )(*sums)
    return got, total


def update(weights, moments, seconds, gradients, total, tiles=8):
    n = len(weights)
    count = 16 * sum(w.size for w in weights)
    flat_all = lambda arrays: [x.reshape(-1, x.shape[-1]) for x in arrays]
    args = [y for x in (weights, moments, seconds, gradients) for y in flat_all(x)]

    def body(total_ref, *refs):
        w_in, m_in, v_in, g_in, w_out, m_out, v_out = (refs[n * i : n * (i + 1)] for i in range(7))
        factor = jnp.minimum(1.0, 0.5 * lax.rsqrt(total_ref[...][:1, :1] / count + 1e-30))
        for i in range(n):
            g, w = g_in[i][...].astype(F32) * factor, w_in[i][...].astype(F32)
            m = 0.9 * m_in[i][...] + 0.1 * g
            v = 0.95 * v_in[i][...] + 0.05 * g * g
            m_out[i][...] = m
            v_out[i][...] = v
            w_out[i][...] = (w - 0.02 * (m * lax.rsqrt(v + 1e-8) + 0.1 * w)).astype(BF16)

    specs = [rows(x.shape[0] // tiles, x.shape[1]) for x in args]
    got = run(body, (tiles,), [total, *args], [once(*total.shape), *specs], specs[: 3 * n], [shape(*x.shape, dtype=x.dtype) for x in args[: 3 * n]])
    return tuple(x.reshape(w.shape) for x, w in zip(got, [*weights] * 3))


def step(x, dy, *arrays):
    wq, wk, wv, wo, gate, up, down = weights = arrays[:7]
    x, dy = x[0], dy[0]
    IDS.clear()
    cos, sin = tables(x.shape[0])
    gathered = lambda w: lax.all_gather(w, "dp", axis=0, tiled=True)
    project, cut = (wq, wk, wv), 6
    hidden = gate.shape[2]
    wo_at = 2 * hidden // wo.shape[2]

    B0 = gathered(jnp.concatenate([gate[0], up[0], wo[0]], -1))
    Wd0 = gathered(down[0])
    B1 = gathered(jnp.concatenate([gate[1], up[1], wo[1]], -1))
    Wd1 = gathered(down[1])
    (W0,) = run(None, (1,), [], [], [], [], jobs=[Fetch(project, 0)])
    a0, q0, k0, v0 = qkv(x, W0, cos, sin)
    o0, lse0 = attend(q0, k0, v0)
    h0, b0 = joined(o0, B0, x, skip=wo_at)
    act0, pu0, pg0, W1 = gated(b0, B0, hidden, [Fetch(project, 1, (1, 2, 3, 7))])
    (h1,) = joined(act0, Wd0, h0, norm=False)
    a1, q1, k1, v1 = qkv(h1, W1, cos, sin)
    o1, lse1 = attend(q1, k1, v1)
    h2, b1 = joined(o1, B1, h1, skip=wo_at)
    act1, pu1, pg1 = gated(b1, B1, hidden)

    (Dd1,) = by_weight(act1, dy)
    *_, Dg1, Du1, dh2, _, _, d1q, _, _, g1q, _, _, u1q = mlp_back(dy, b1, B1, Wd1, pu1, pg1, h2, chained([Dd1]), cut)
    do1, Do1, g1p, u1p = projected_back(dh2, o1, B1, wo_at, [Pair([Dg1]), Pair([Du1])])
    halves = Half([Dg1], g1p), Half([Du1], u1p)
    dq1, dk1, dv1, *_, e1q, f1q, o1p = attend_back(q1, k1, v1, o1, do1, lse1, cos, sin, [
        *halves, Quad([Dg1], g1p, halves[0], at_once(3)), Quad([Du1], u1p, halves[1], at_once(5)), Pair([Do1])])
    *D1, o1h = by_weights(a1, [dq1, dk1, dv1], [Half([Do1], o1p)], tn=HEAD)
    dh1, o1q, a1p = by_input([dq1, dk1, dv1], [(w, 0) for w in W1], h1, dh2, [Quad([Do1], o1p, o1h), Pair(D1)])

    Dd0, a1h = by_weight(act0, dh1, [Half(D1, a1p)])
    *_, Dg0, Du0, dh0, a1q, _, _, d0q, _, _, g0q, _, _, u0q = mlp_back(dh1, b0, B0, Wd0, pu0, pg0, h0, [Quad(D1, a1p, a1h), *chained([Dd0])], cut)
    do0, Do0, g0p, u0p = projected_back(dh0, o0, B0, wo_at, [Pair([Dg0]), Pair([Du0])])
    halves = Half([Dg0], g0p), Half([Du0], u0p)
    dq0, dk0, dv0, _, _, e0q, f0q, o0p, o0h = attend_back(q0, k0, v0, o0, do0, lse0, cos, sin, [
        *halves, Quad([Dg0], g0p, halves[0], at_once(3)), Quad([Du0], u0p, halves[1], at_once(5)), *chained([Do0])[:2]])
    a0s, o0q = last_weights(a0, [dq0, dk0, dv0], [Quad([Do0], o0p, o0h)])

    moved = lambda quad: [(n, pl.ds(c.start + cut * HEAD, c.size), *sums) for n, c, *sums in quad]
    layer0 = [*a0s, o0q, g0q + moved(e0q), u0q + moved(f0q), d0q]
    layer1 = [*([part] for part in a1q), o1q, g1q + moved(e1q), u1q + moved(f1q), d1q]
    return update(weights, arrays[7:14], arrays[14:21], *join(list(zip(layer0, layer1)), [w.shape for w in weights]))


def solution(mesh):
    states, cut = P(("rep", "dp"), None, None), P(None, "dp", None)
    return jax.shard_map(
        step,
        mesh=mesh,
        in_specs=(states, states) + (cut,) * 21,
        out_specs=(P("rep", "dp", None),) * 21,
        check_vma=False,
    )
```

```python
import jax
import jax.numpy as jnp
from jax import lax
from jax.experimental import pallas as pl
from jax.experimental.pallas import tpu as pltpu
from jax.sharding import PartitionSpec as P

F32, BF16 = jnp.float32, jnp.bfloat16
MESH = pl.DeviceIdType.MESH
ANY = pl.BlockSpec(memory_space=pl.ANY)
DMA, VM = pltpu.SemaphoreType.DMA, pltpu.VMEM
LIMIT = 62 * 2**20
WORK = 2 * 10**10
WIDE = 512
HEAD = 256
HEADS = 4
THETA = 10000
LOG2E = 1.4426950408889634
NEG = -1e30
HIDDEN = 2 * NEG
DIMS = (8, 4, 2)
CORE = 1
ALL = slice(None)
EACH = range(3)
CUBE = (2, 2, 2, 2)


def dot(a, b, ca, cb):
    return lax.dot_general(a, b, (((ca,), (cb,)), ((), ())), preferred_element_type=F32)


def nn(a, b):
    return dot(a, b, 1, 0)


def nt(a, b):
    return dot(a, b, 1, 1)


def tt(a, b):
    return dot(a, b, 0, 0)


def shape(*size, dtype=BF16):
    return jax.ShapeDtypeStruct(size, dtype)


def chunk(n, size):
    return pl.ds(pl.multiple_of(n * size, size), size)


def loop(count, what):
    lax.fori_loop(0, count, lambda n, _: what(n), None)


def bit(mask):
    return lax.rem(lax.axis_index("dp") // mask, 2)


def peer(mask):
    at = lax.axis_index("dp")
    for m in (*DIMS, CORE):
        if mask & m:
            at = at + m - 2 * m * bit(m)
    return {"dp": at}


def place():
    return [bit(m) for m in DIMS]


def among(p, at):
    return tuple(at if n == p else ALL for n in EACH)


def parts_of(arrays):
    size = arrays[0].shape[-1]
    if len(arrays) > 1:
        return [(n, pl.ds(0, size)) for n in EACH]
    unit = size // 128
    wide = -(-unit // 3)
    return [(0, pl.ds(128 * wide * n, 128 * min(wide, unit - wide * n))) for n in EACH]


def remote(src, dst, sems, n, mask):
    return pltpu.make_async_remote_copy(src_ref=src, dst_ref=dst, send_sem=sems[0].at[n], recv_sem=sems[1].at[n], device_id=peer(mask), device_id_type=MESH)


def local(src, dst, sems, n):
    return pltpu.make_async_copy(src, dst, sems.at[n])


def start_all(copies):
    for c in copies:
        c.start()


def wait_all(copies):
    for c in copies:
        c.wait()


def flat(ref):
    size = 1
    for n in ref.shape[:-1]:
        size *= n
    return ref.reshape(size, ref.shape[-1])


def added(into, others, size=64):
    into, others = flat(into), [flat(o) for o in others]

    def some(n):
        at = chunk(n, size)
        total = into[at, :].astype(F32)
        for o in others:
            total = total + o[at, :].astype(F32)
        into[at, :] = total.astype(BF16)

    loop(into.shape[0] // size, some)


class Fetch:
    masks = (*DIMS, CORE)

    def __init__(self, ws, layer, at=(1, 3, 5, 7)):
        _, self.rows, self.columns = ws[0].shape
        self.layer, self.at, self.ins, k = layer, at, list(ws), len(ws)
        self.outs = [shape(*CUBE, self.rows, self.columns)] * k
        self.scratch = [VM((k, self.rows, self.columns), BF16), DMA((2 * k,)), DMA((21,)), DMA((21,))]
        self.parts = parts_of(ws)

    def done(self, outs):
        return [o.reshape(16 * self.rows, self.columns) for o in outs]

    def stages(self, ws, fulls, scratch):
        own, sem, *sems = scratch
        b, core, k = place(), bit(CORE), len(ws)
        loads = lambda: [local(w.at[self.layer], own.at[n], sem, n) for n, w in enumerate(ws)]
        keeps = lambda: [local(own.at[n], full.at[(*b, core)], sem, k + n) for n, full in enumerate(fulls)]
        axis = lambda p, level: (p + 2 - level) % 3

        def held(p, level, other=None):
            which, columns = self.parts[p]
            idx = list(b)
            for n in range(level):
                idx[axis(p, n)] = ALL
            if other:
                idx[axis(p, level)] = 1 - b[axis(p, level)]
            return fulls[which].at[(*idx, core, ALL, columns)]

        def first_of(p):
            which, columns = self.parts[p]
            return own.at[which, :, columns]

        def across(p, level):
            return remote(held(p, level) if level else first_of(p), held(p, level), sems, 3 * level + p, DIMS[axis(p, level)])

        def pair(p, level):
            if not level:
                return remote(first_of(p), held(p, level), sems, 9 + p, CORE)
            got = held(p, level - 1, True)
            return remote(got, got, sems, 9 + 3 * level + p, CORE)

        def begin():
            start_all(loads())

        def first():
            wait_all(loads())
            start_all(keeps())
            start_all([across(p, 0) for p in EACH] + [pair(p, 0) for p in EACH])

        def next_of(level):
            def go():
                if level == 1:
                    wait_all(keeps())
                for p in EACH:
                    across(p, level - 1).wait_recv()
                    if level < 3:
                        across(p, level).start()
                    pair(p, level).start()

            return go

        def end():
            for p in EACH:
                for level in EACH:
                    across(p, level).wait_send()
                wait_all([pair(p, level) for level in range(4)])

        return [(0, begin), *zip(self.at, (first, *(next_of(n + 1) for n in EACH))), (None, end)]


def cube(g):
    return g if len(g.shape) > len(CUBE) else g.reshape(*CUBE, g.shape[0] // 16, g.shape[1])


class Mine:
    def __init__(self, index, *size):
        self.index, self.shape = index, size


def given(arrays):
    return [x for x in arrays if not isinstance(x, Mine)] if isinstance(arrays, list) else []


def gradients_of(job, refs):
    n = len(given(job.grads))
    return refs[:n] or [job.outer[g.index] for g in job.grads], refs[n:]


class Pair:
    masks = (CORE,)
    followed = None

    def __init__(self, grads, at=1):
        self.grads = [cube(g) for g in grads]
        self.at, self.ins = at, given(self.grads)
        self.outs = [shape(*CUBE[1:], *g.shape[4:]) for g in self.grads]
        self.scratch = [DMA((len(grads),))] * 2

    def done(self, outs):
        return outs

    def stages(self, ins, outs, sems):
        self.refs = outs
        grads, _ = gradients_of(self, ins)
        self.copies = lambda: [remote(g.at[:, :, :, 1 - bit(CORE)], r, sems, n, CORE) for n, (g, r) in enumerate(zip(grads, outs))]
        return [(self.at, lambda: start_all(self.copies())), (None, lambda: left(self))]


def left(job):
    for c in job.copies():
        if job.followed:
            c.wait_send()
        else:
            c.wait()


def follow(before, refs):
    if isinstance(before, list):
        return refs, lambda: None
    before.followed = True

    def arrive():
        for c in before.copies():
            c.wait_recv()

    return before.refs, arrive


class Half:
    masks = DIMS
    followed = None

    def __init__(self, grads, pairs, at=(0, 1, 1)):
        self.at, self.grads, self.parts, self.pairs = at, [*map(cube, grads)], parts_of(grads), pairs
        self.ins = [*given(self.grads), *given(pairs)]
        self.sizes = [(2, 2, self.grads[0].shape[4], c.size) for _, c in self.parts]
        self.outs = [shape(*s) for s in self.sizes]
        self.scratch = [VM(s, BF16) for s in self.sizes] * 2 + [DMA((6,)), DMA((3,)), DMA((3,))]

    def done(self, outs):
        return outs

    def stages(self, ins, outs, scratch):
        grads, ins = gradients_of(self, ins)
        pairs, arrive = follow(self.pairs, ins)
        a, r, (sem, *sems) = scratch[:3], scratch[3:6], scratch[6:]
        self.refs, self.spare = outs, r

        def loads():
            got = []
            for p, (n, columns) in enumerate(self.parts):
                at = among(p, 1 - bit(DIMS[p]))
                got.append(local(grads[n].at[(*at, bit(CORE), ALL, columns)], a[p], sem, p))
                got.append(local(pairs[n].at[(*at, ALL, columns)], r[p], sem, 3 + p))
            return got

        def begin():
            arrive()
            start_all(loads())

        def add():
            wait_all(loads())
            for p in EACH:
                added(a[p], [r[p]])

        self.copies = lambda: [remote(a[p], outs[p], sems, p, DIMS[p]) for p in EACH]
        return [*zip(self.at, (begin, add, lambda: start_all(self.copies()))), (None, lambda: left(self))]


class Quad:
    masks = (2, 4, 6, 8, 10, 12)

    def __init__(self, grads, pairs, halves, at=(0, 1, 1)):
        self.at, self.grads, self.parts, self.pairs, self.halves = at, [*map(cube, grads)], parts_of(grads), pairs, halves
        self.ins = [*given(self.grads), *given(pairs), *given(halves)]
        rows = self.grads[0].shape[4]
        self.outs = [shape(rows, c.size, dtype=F32) for _, c in self.parts] + [shape(3, rows, c.size) for _, c in self.parts]
        self.scratch = [VM((2, 2, rows, c.size), BF16) for _, c in self.parts] * (3 if given(halves) else 2) + [VM((rows, c.size), F32) for _, c in self.parts]
        self.scratch += [DMA((12,)), DMA((9,)), DMA((9,))]

    def done(self, outs):
        return [(*part, *sums) for part, *sums in zip(self.parts, outs[:3], outs[3:])]

    def stages(self, ins, outs, scratch):
        grads, ins = gradients_of(self, ins)
        m = len(given(self.pairs))
        pairs, _ = follow(self.pairs, ins[:m])
        halves, arrive = follow(self.halves, ins[m:])
        sem, *sems = scratch[-3:]
        a, s, own, r = scratch[:3], scratch[3:6], scratch[-6:-3], getattr(self.halves, "spare", scratch[6:9])

        def loads():
            got = []
            for p, (n, columns) in enumerate(self.parts):
                at = among(p, bit(DIMS[p]))
                got.append(local(grads[n].at[(*at, bit(CORE), ALL, columns)], a[p], sem, p))
                got.append(local(pairs[n].at[(*at, ALL, columns)], r[p], sem, 3 + p))
                got.append(local(halves[p], s[p], sem, 6 + p))
            return got

        def begin():
            arrive()
            start_all(loads())

        def add():
            wait_all(loads())
            for p in EACH:
                total_of(p, own[p], a[p], r[p], s[p])
                added(a[p], [r[p], s[p]])

        copies = lambda: [local(own[p], outs[p], sem, 9 + p) for p in EACH] + [c for p in EACH for c in to_three(p, a[p], outs[3 + p], sems)]
        return [*zip(self.at, (begin, add, lambda: start_all(copies()))), (None, lambda: wait_all(copies()))]


def chained(grads, ready=0, third=4):
    pair = Pair(grads, ready + 1)
    half = Half(grads, pair, at_once(ready + 3))
    return [pair, half, Quad(grads, pair, half, at_once(ready + 3 + third))]


def at_once(n):
    return n, n + 1, n + 1


def sides(p):
    u, v = (n for n in EACH if n != p)
    return u, v, bit(DIMS[u]), bit(DIMS[v])


def total_of(p, own, *terms, size=64):
    _, _, bu, bv = sides(p)

    def some(n):
        at = chunk(n, size)
        own[at, :] = sum(x[bu, bv, at, :].astype(F32) for x in terms)

    loop(own.shape[0] // size, some)


def to_three(p, blocks, others, sems, base=0):
    u, v, bu, bv = sides(p)
    flips = ((1, 0), (0, 1), (1, 1))
    return [remote(blocks.at[1 - bu if fu else bu, 1 - bv if fv else bv], others.at[n], sems, base + 3 * p + n, DIMS[u] * fu + DIMS[v] * fv)
            for n, (fu, fv) in enumerate(flips)]


IDS = []


def talk():
    IDS.append(None)
    return dict(collective_id=len(IDS), has_side_effects=True)


def hello(masks):
    for m in masks:
        pl.semaphore_signal(pltpu.get_barrier_semaphore(), inc=1, device_id=peer(m), device_id_type=MESH)


def met(masks):
    pl.semaphore_wait(pltpu.get_barrier_semaphore(), len(masks))


def run(body, grid, args, in_specs, out_specs, out_shapes, scratch=(), jobs=()):
    steps = 1
    for g in grid:
        steps *= g
    gather = lambda name: [x for job in jobs for x in getattr(job, name)]
    ins, outs, scr = gather("ins"), gather("outs"), gather("scratch")
    masks = sorted(set(gather("masks")))

    def kernel(*refs):
        refs = list(refs)
        take = lambda held, n: [held.pop(0) for _ in range(n)]
        my_in, job_in, my_out, job_out, my_scr, job_scr = (take(refs, len(x)) for x in (args, ins, out_shapes, outs, scratch, scr))
        step = 0
        for axis, g in enumerate(grid):
            step = step * g + pl.program_id(axis)
        plan = {}
        for job in jobs:
            job.outer = my_out
            for at, what in job.stages(take(job_in, len(job.ins)), take(job_out, len(job.outs)), take(job_scr, len(job.scratch))):
                plan.setdefault(at if at is None else min(at, steps - 1), []).append(what)
        last = plan.pop(None, [])
        if jobs:
            plan.setdefault(0, []).insert(0, lambda: hello(masks))
            greet = min(1, steps - 1)
            plan.setdefault(greet, []).insert(1 - greet, lambda: met(masks))
        for at in sorted(plan):

            @pl.when(step == at)
            def _(todo=plan[at]):
                for what in todo:
                    what()

        if body is not None:
            body(*my_in, *my_out, *my_scr)
        if last:

            @pl.when(step == steps - 1)
            def _():
                for what in last:
                    what()

    got = list(pl.pallas_call(
        kernel,
        grid=grid,
        in_specs=[*in_specs, *[ANY] * len(ins)],
        out_specs=[*out_specs, *[ANY] * len(outs)],
        out_shape=[*out_shapes, *outs],
        scratch_shapes=[*scratch, *scr],
        compiler_params=pltpu.CompilerParams(dimension_semantics=("arbitrary",) * len(grid), vmem_limit_bytes=LIMIT, **(talk() if jobs else {})),
        cost_estimate=pl.CostEstimate(flops=WORK, bytes_accessed=sum(x.size * x.dtype.itemsize for x in args), transcendentals=0),
    )(*args, *ins))
    mine = [got.pop(0) for _ in out_shapes]
    return (*mine, *(job.done([got.pop(0) for _ in job.outs]) for job in jobs))


block = pl.BlockSpec


def columns(size, tile, skip=0):
    return block((size, tile), lambda j: (0, j + skip))


def slices(size, tile):
    return [slice(n, n + tile) for n in range(0, size, tile)]


def rows(tile, size):
    return block((tile, size), lambda i: (i, 0))


def once(*size):
    return block(size, lambda *_: (0,) * len(size), pipeline_mode=pl.Buffered(1))


class Sum:
    masks = (CORE, *DIMS, 6, 10, 12)

    def __init__(self, grads, at=(0, 1, 2, 4)):
        self.at, self.ins = at, [*map(cube, grads)]
        self.parts = parts_of(grads)
        self.outs = [shape(*g.shape[4:]) for g in self.ins]
        self.scratch = [VM(g.shape, BF16) for g in self.ins] + chain_scratch(self.ins[0].shape[4], self.parts) + [DMA((len(grads),))]

    def done(self, outs):
        return outs

    def stages(self, ins, outs, scratch):
        held, sem = scratch[: len(ins)], scratch[-1]
        core = bit(CORE)
        mine = lambda: [local(g.at[:, :, :, core], h.at[:, :, :, core], sem, n) for n, (g, h) in enumerate(zip(ins, held))]
        pair, half, quad, end = chain([(ins[n], held[n], outs[n], c) for n, c in self.parts], scratch[len(ins) : -1])

        def loaded():
            wait_all(mine())
            half()

        return [*zip(self.at, (lambda: start_all(mine()), pair, loaded, quad)), (None, end)]


def chain_scratch(rows, parts):
    wide = [c.size for _, c in parts]
    return ([VM((2, 2, 2, rows, w), BF16) for w in wide] + [VM((2, 2, rows, w), BF16) for w in wide] * 2 + [VM((3, rows, w), BF16) for w in wide]
            + [VM((rows, w), F32) for w in wide] + [VM((rows, w), BF16) for w in wide] + [DMA((15,))] * 2 + [DMA((3,))])


def chain(parts, scratch):
    (r, s, t, o, own, res), (send, recv, keep) = [scratch[3 * i : 3 * i + 3] for i in range(6)], scratch[18:]
    core = bit(CORE)

    sems = (send, recv)
    to_core = lambda: [remote(src.at[:, :, :, 1 - core, :, c], r[p], sems, p, CORE) for p, (src, _, _, c) in enumerate(parts)]
    to_next = lambda: [remote(s[p], t[p], sems, 3 + p, DIMS[p]) for p in EACH]
    to_rest = lambda: [c for p in EACH for c in to_three(p, s[p], o[p], sems, 6)]
    keeps = lambda: [local(res[p], out.at[:, c], keep, p) for p, (_, _, out, c) in enumerate(parts)]

    def both(p, place, i, j):
        xyz = [i, j]
        xyz.insert(p, place)
        _, held, _, c = parts[p]
        return held[(*xyz, core, ALL, c)].astype(F32) + r[p][tuple(xyz)].astype(F32)

    def half():
        for c in to_core():
            c.wait_recv()
        for p in EACH:

            def some(n, p=p):
                i, j = n // 2, lax.rem(n, 2)
                s[p][i, j] = both(p, 1 - bit(DIMS[p]), i, j).astype(BF16)

            loop(4, some)
        start_all(to_next())

    def quad():
        for c in to_next():
            c.wait()
        for p in EACH:
            u, v, bu, bv = sides(p)

            def some(n, p=p):
                i, j = n // 2, lax.rem(n, 2)
                s[p][i, j] = (both(p, bit(DIMS[p]), i, j) + t[p][i, j].astype(F32)).astype(BF16)

            own[p][...] = both(p, bit(DIMS[p]), bu, bv) + t[p][bu, bv].astype(F32)
            loop(4, some)
        start_all(to_rest())

    def end():
        for c in to_core():
            c.wait_send()
        wait_all(to_rest())
        for p in EACH:
            res[p][...] = (own[p][...] + sum(o[p][n].astype(F32) for n in EACH)).astype(BF16)
        start_all(keeps())
        wait_all(keeps())

    return lambda: start_all(to_core()), half, quad, end


def unit(h):
    wide = h.astype(F32)
    return wide, lax.rsqrt(jnp.mean(wide * wide, -1, keepdims=True) + 1e-6)


def normed(h):
    wide, scale = unit(h)
    return (wide * scale).astype(BF16)


def unit_back(h, by_normed, by_h):
    wide, scale = unit(h)
    d = by_normed.astype(BF16).astype(F32)
    d = scale * d - wide * (scale * scale * scale * jnp.mean(d * wide, -1, keepdims=True))
    return (by_h.astype(F32) + d.astype(BF16).astype(F32)).astype(BF16)


def turned(t, cos, sin):
    half = t.shape[1] // 2
    a, b = t[:, :half], t[:, half:]
    return jnp.concatenate([a * cos - b * sin, b * cos + a * sin], -1)


def tables(tokens):
    half = HEAD // 2
    angle = jnp.arange(tokens, dtype=F32)[:, None] * THETA ** (-jnp.arange(half, dtype=F32) / half)
    return jnp.cos(angle), jnp.sin(angle)


def head(i):
    return slice(i * HEAD, (i + 1) * HEAD)


def qkv(h, w, cos, sin, jobs=(), tm=HEAD):
    t, d = h.shape
    n = w[0].shape[1]

    def body(h_ref, wq, wk, wv, cos_ref, sin_ref, a_ref, q_ref, k_ref, v_ref):
        a = normed(h_ref[...])
        a_ref[...] = a
        v_ref[...] = nn(a, wv[...]).astype(BF16)
        for w_ref, o_ref in ((wq, q_ref), (wk, k_ref)):
            y = nn(a, w_ref[...]).astype(BF16)
            for i in range(n // HEAD):
                o_ref[:, head(i)] = turned(y[:, head(i)].astype(F32), cos_ref[...], sin_ref[...]).astype(BF16)

    part, angle = rows(tm, n), rows(tm, HEAD // 2)
    return run(body, (t // tm,), [h, *w, cos, sin], [rows(tm, d), *[once(d, n)] * 3, angle, angle], [rows(tm, d), part, part, part],
               [shape(t, d), *[shape(t, n)] * 3], jobs=jobs)


def gap(bk, bq):
    return lax.broadcasted_iota(jnp.int32, (bk, bq), 1) - lax.broadcasted_iota(jnp.int32, (bk, bq), 0)


def blocks_of(iq, bq, bk, one):
    per = bq // bk
    loop(iq * per, lambda j: one(j, None))
    lax.fori_loop(iq * per, iq * per + per, lambda j, _: one(j, j * bk - iq * bq), None)


def attend(q, k, v, jobs=(), bq=WIDE, bk=WIDE, strip=WIDE):
    t, n = q.shape
    scale = HEAD**-0.5
    e = scale * LOG2E
    pieces = [(i, at) for i in range(HEADS) for at in slices(bq, strip)]

    def body(q_ref, k_ref, v_ref, o_ref, lse_ref, top_s, mix_s):
        top_s[...] = jnp.full(top_s.shape, NEG, F32)
        mix_s[...] = jnp.zeros(mix_s.shape, F32)
        ones = jnp.ones((8, bk), BF16)

        def one(j, hidden):
            here = chunk(j, bk)
            scores = [nt(k_ref[here, head(i)], q_ref[at, head(i)]) for i, at in pieces]
            weights, keeps = [], []
            for (i, at), s in zip(pieces, scores):
                if hidden is not None:
                    s = jnp.where(gap(bk, strip) >= hidden - at.start, s, HIDDEN)
                old = top_s[pl.ds(i, 1), at]
                top = jnp.maximum(old, s.max(axis=0, keepdims=True))
                top_s[pl.ds(i, 1), at] = top
                weights.append(jnp.exp2((s - top) * e).astype(BF16))
                keeps.append(jnp.exp2((old - top) * e))
            for (i, at), p, keep in zip(pieces, weights, keeps):
                values = jnp.concatenate([v_ref[here, head(i)].T, ones], axis=0)
                mix_s[i, :, at] = mix_s[i, :, at] * keep + nn(values, p)

        blocks_of(pl.program_id(0), bq, bk, one)
        for i in range(HEADS):
            total = mix_s[i, HEAD : HEAD + 1, :]
            o_ref[:, head(i)] = (mix_s[i, :HEAD, :] * (1 / total)).T.astype(BF16)
            lse_ref[pl.ds(i, 1), :] = top_s[pl.ds(i, 1), :] * scale + jnp.log(total)

    part = rows(bq, n)
    return run(body, (t // bq,), [q, k, v], [part, once(t, n), once(t, n)], [part, columns(HEADS, bq)],
               [shape(t, n), shape(HEADS, t, dtype=F32)], [VM((HEADS, bq), F32), VM((HEADS, HEAD + 8, bq), F32)],
               jobs=jobs)


def attend_back(q, k, v, out, by_out, lse, cos, sin, jobs=(), bq=WIDE, bk=WIDE, strip=WIDE, together=2):
    t, n = q.shape
    scale = HEAD**-0.5
    e = scale * LOG2E
    width = together * HEAD
    nq = t // bq
    pieces = [(i, at) for i in range(together) for at in slices(bq, strip)]

    def back(d, cos, sin):
        return turned(d.astype(BF16).astype(F32), cos, -sin).astype(BF16)

    def body(q_ref, k_ref, v_ref, o_ref, do_ref, lse_ref, cos_ref, sin_ref, dq_ref, dk_ref, dv_ref, dq_s, dk_s, dv_s, lse_s, delta_s):
        first, iq = pl.program_id(0) * together, pl.program_id(1)

        @pl.when(iq == 0)
        def _():
            dk_s[...] = jnp.zeros(dk_s.shape, F32)
            dv_s[...] = jnp.zeros(dv_s.shape, F32)

        dq_s[...] = jnp.zeros(dq_s.shape, F32)
        for i in range(together):
            lse_s[pl.ds(i, 1), :] = lse_ref[pl.ds(first + i, 1), :] * LOG2E
            both = do_ref[:, head(i)].astype(F32) * o_ref[:, head(i)].astype(F32)
            delta_s[pl.ds(i, 1), :] = (both[:, : HEAD // 2] + both[:, HEAD // 2 :]).T.sum(axis=0, keepdims=True)

        def one(j, hidden):
            here = chunk(j, bk)
            scores = [nt(k_ref[here, head(i)], q_ref[at, head(i)]) for i, at in pieces]
            dps = [nt(v_ref[here, head(i)], do_ref[at, head(i)]) for i, at in pieces]
            for (i, at), s, dp in zip(pieces, scores, dps):
                p = jnp.exp2(s * e - lse_s[pl.ds(i, 1), at])
                if hidden is not None:
                    p = jnp.where(gap(bk, strip) >= hidden - at.start, p, 0.0)
                ds = (p * (dp - delta_s[pl.ds(i, 1), at])).astype(BF16)
                dv_s[here, head(i)] += nn(p.astype(BF16), do_ref[at, head(i)])
                dk_s[here, head(i)] += nn(ds, q_ref[at, head(i)])
                dq_s[i, :, at] += nn(k_ref[here, head(i)].T, ds)

        blocks_of(iq, bq, bk, one)
        these = chunk(iq, bq)
        for i in range(together):
            dq_ref[:, head(i)] = back((dq_s[i] * scale).T, cos_ref[these, :], sin_ref[these, :])

        @pl.when(iq == nq - 1)
        def _():
            def some(m):
                at = chunk(m, HEAD)
                for i in range(together):
                    dk_ref[at, head(i)] = back(dk_s[at, head(i)] * scale, cos_ref[at, :], sin_ref[at, :])
                dv_ref[at, :] = dv_s[at, :].astype(BF16)

            loop(t // HEAD, some)

    part = block((bq, width), lambda h, i: (i, h))
    whole = block((t, width), lambda h, i: (0, h))
    angle = once(t, HEAD // 2)
    return run(body, (n // width, nq), [q, k, v, out, by_out, lse, cos, sin],
               [part, whole, whole, part, part, block((HEADS, bq), lambda h, i: (0, i)), angle, angle], [part, whole, whole], [shape(t, n)] * 3,
               [VM((together, HEAD, bq), F32), VM((t, width), F32), VM((t, width), F32), VM((8, bq), F32), VM((8, bq), F32)],
               jobs=jobs)


def joined(a, w, place, h, jobs=(), tm=WIDE, norm=True):
    t, n = h.shape
    k = a.shape[1]

    def body(a_ref, w_ref, h_ref, o_ref, *b_ref):
        y = nn(a_ref[...], w_ref[...].reshape(k, n)).astype(BF16)
        new = (h_ref[...].astype(F32) + y.astype(F32)).astype(BF16)
        o_ref[...] = new
        for ref in b_ref:
            ref[...] = normed(new)

    outs = [rows(tm, n)] * (1 + norm)
    return run(body, (t // tm,), [a, w, h], [rows(tm, k), block((16, k // 16, n), lambda i: (0, *place), pipeline_mode=pl.Buffered(1)), rows(tm, n)], outs, [shape(t, n) for _ in outs], jobs=jobs)


def gated(b, both, n, jobs=(), tn=WIDE, sub=WIDE):
    t, d = b.shape

    def body(b_ref, g_ref, u_ref, act_ref, by_u, by_g):
        for at in slices(t, sub):
            g, u = nn(b_ref[at, :], g_ref[...]), nn(b_ref[at, :], u_ref[...])
            s = jax.nn.sigmoid(g)
            p = g * s
            by_u[at, :] = p
            by_g[at, :] = u * (s + p * (1 - s))
            act_ref[at, :] = (p * u).astype(BF16)

    tile = columns(t, tn)
    return run(body, (n // tn,), [b, both, both], [once(t, d), columns(d, tn), columns(d, tn, n // tn)], [tile] * 3,
               [shape(t, n), shape(t, n, dtype=F32), shape(t, n, dtype=F32)], jobs=jobs)


def mlp_back(by_h, b, both, down, by_u, by_g, h, jobs, cut, tn=HEAD, sub=WIDE):
    t, d = by_h.shape
    n = by_u.shape[1]
    tiles = n // tn
    sizes = [(*CUBE, d // 16, tn * k) for k in (cut, cut, tiles - cut, tiles - cut)]

    def body(dh_ref, b_ref, wg_ref, wu_ref, wd_ref, pu_ref, pg_ref, h_ref, *refs):
        *outs, out, dg_s, du_s, total, mine, up_s, gate_s, sem = refs
        staged = gate_s, up_s
        j = pl.program_id(0)

        def stores(outs, skip):
            return [local(x, o.at[(*[ALL] * 5, chunk(j - skip, tn))], sem, i) for i, (x, o) in enumerate(zip(staged, outs))]

        @pl.when(j == 0)
        def _():
            total[...] = jnp.zeros(total.shape, F32)

        cuts = slices(t, sub)
        for at in cuts:
            da = nt(dh_ref[at, :], wd_ref[0]).astype(BF16).astype(F32)
            du_s[at, :] = (da * pu_ref[at, :]).astype(BF16)
            dg_s[at, :] = (da * pg_ref[at, :]).astype(BF16)
        for at in cuts:
            total[at, :] += nt(dg_s[at, :], wg_ref[...]) + nt(du_s[at, :], wu_ref[...])

        @pl.when(j > 0)
        def _():
            wait_all(stores(outs, j))

        for x, s in zip((dg_s, du_s), staged):
            s[...] = tt(b_ref[...], x[...]).astype(BF16).reshape(s.shape)

        @pl.when(j < cut)
        def _():
            start_all(stores(outs, 0))

        @pl.when(j >= cut)
        def _():
            start_all(stores(outs[2:], cut))

        @pl.when(j == tiles - 1)
        def _():
            def some(m):
                at = chunk(m, tn)
                mine[at, :] = unit_back(h_ref[at, :], total[at, :], dh_ref[at, :])

            loop(t // tn, some)
            last = [local(mine, out, sem, len(outs)), *stores(outs, j)]
            last[0].start()
            wait_all(last)

    tile = columns(t, tn)
    whole = once(t, d)
    return run(body, (tiles,), [by_h, b, both, both, down, by_u, by_g, h],
               [whole, whole, columns(d, tn), columns(d, tn, tiles), block((1, tn, d), lambda j: (j, 0, 0)), tile, tile, whole], [ANY] * 5,
               [*[shape(*s) for s in sizes], shape(t, d)],
               [VM((t, tn), BF16), VM((t, tn), BF16), VM((t, d), F32), VM((t, d), BF16), *[VM((*CUBE, d // 16, tn), BF16)] * 2, DMA((5,))],
               jobs=[*jobs, *(c for i in (0, 1) for c in chained([Mine(i, *sizes[i])], cut))])


def by_weight(a, d, jobs=(), tm=WIDE):
    t, m = a.shape
    n = d.shape[1]

    def body(a_ref, d_ref, o_ref):
        o_ref[...] = tt(a_ref[...], d_ref[...]).astype(BF16)

    return run(body, (m // tm,), [a, d], [columns(t, tm), once(t, n)], [rows(tm, n)], [shape(m, n)], jobs=jobs)


def by_weights(a, ds, jobs=(), tn=WIDE):
    t, m = a.shape
    n = ds[0].shape[1]
    k = len(ds)

    def body(a_ref, *refs):
        for d_ref, o_ref in zip(refs[:k], refs[k:]):
            o_ref[...] = tt(a_ref[...], d_ref[...]).astype(BF16)

    return run(body, (n // tn,), [a, *ds], [once(t, m), *[columns(t, tn)] * k], [columns(m, tn)] * k, [shape(m, n)] * k, jobs=jobs)


def by_input(ds, ws, h, by_h, jobs=(), tm=HEAD):
    t, n = h.shape
    k = len(ds)

    def body(*refs):
        h_ref, dh_ref, o_ref = refs[2 * k :]
        total = sum(nt(d[...], w[...]) for d, w in zip(refs[:k], refs[k : 2 * k]))
        o_ref[...] = unit_back(h_ref[...], total, dh_ref[...])

    specs = [block((n, d.shape[1]), lambda i, skip=skip: (0, skip), pipeline_mode=pl.Buffered(1)) for d, (_, skip) in zip(ds, ws)]
    return run(body, (t // tm,), [*ds, *[w for w, _ in ws], h, by_h], [*[rows(tm, d.shape[1]) for d in ds], *specs, rows(tm, n), rows(tm, n)], [rows(tm, n)],
               [shape(t, n)], jobs=jobs)


def projected_back(by_h, a, w, place, jobs=(), tn=HEAD):
    t, d = by_h.shape
    n = a.shape[1]

    def body(dh_ref, a_ref, w_ref, da_ref, dw_ref):
        da_ref[...] = nt(dh_ref[...], w_ref[...].reshape(tn, d)).astype(BF16)
        dw_ref[...] = tt(a_ref[...], dh_ref[...]).astype(BF16)

    tile = columns(t, tn)
    return run(body, (n // tn,), [by_h, a, w], [once(t, d), tile, block((16 * tn // n, n // 16, d), lambda j: (j, *place))], [tile, rows(tn, d)], [shape(t, n), shape(n, d)], jobs=jobs)


def last_weights(a, ds, jobs=(), tn=WIDE):
    t, m = a.shape
    n = ds[0].shape[1]
    r, k, cut = m // 16, len(ds), n // tn
    steps = k * cut
    masks = Sum.masks
    unit = n // 128
    parts = []
    for turn in range(k):
        wide = [-(-unit // 3)] * 3
        wide[turn] = unit - 2 * wide[turn]
        parts.append([pl.ds(128 * sum(wide[:p]), 128 * wide[p]) for p in EACH])
    sizes = [chain_scratch(r, [(None, c) for c in own]) for own in parts]

    class Chain:
        ins = ()

        def __init__(self):
            self.masks = masks
            self.outs = [shape(r, n)] * k
            self.scratch = [VM((*CUBE, r, n), BF16)] * k + [x for own in sizes for x in own]

        def done(self, outs):
            return outs

        def stages(self, ins, outs, scratch):
            self.held, scratch, self.steps = scratch[:k], scratch[k:], []
            for i in range(k):
                mine = scratch[len(sizes[0]) * i : len(sizes[0]) * (i + 1)]
                self.steps.append(chain([(self.held[i], self.held[i], outs[i], c) for c in parts[i]], mine))
            got = []
            for i, (pair, half, quad, _) in enumerate(self.steps[:-1]):
                at = cut * (i + 1)
                got += [(at, pair), (at + 1, half)] + [(at + 3, quad)] * (at + 3 < steps)
            return [*got, (None, self.rest)]

        def rest(self):
            *_, (_, _, before, _), (pair, half, quad, _) = self.steps
            for what in (pair, before, half, quad, *(s[-1] for s in self.steps)):
                what()

    work = Chain()

    def body(a_ref, *refs):
        j = pl.program_id(0)
        for i in range(k):

            @pl.when(j // cut == i)
            def _(i=i):
                at = chunk(lax.rem(j, cut), tn)
                work.held[i][:, :, :, :, :, at] = tt(a_ref[...], refs[i][...]).astype(BF16).reshape(*CUBE, r, tn)

    specs = [block((t, tn), lambda j, i=i: (0, jnp.clip(j - cut * i, 0, cut - 1))) for i in range(k)]
    return run(body, (steps,), [a, *ds], [once(t, m), *specs], [], [], jobs=[work, *jobs])


def join(gradients, sizes):
    pieces = [(i, layer, *p) for i, of in enumerate(gradients) for layer, g in enumerate(of)
              for p in (g if isinstance(g, list) else [(None, pl.ds(0, sizes[i][2]), g)])]
    sums = []
    for _, _, _, _, *arrays in pieces:
        sums += arrays
    others = range(1, 16)
    n = len(sizes)

    def kernel(*refs):
        refs = list(refs)
        take = lambda n: [refs.pop(0) for _ in range(n)]
        s_in, g_out, (total_out,), g_s, r_s = take(len(sums)), take(n), take(1), take(n), take(len(sums))
        acc, tiles, sem, out_sem, send, recv = refs
        hello(others)
        loads = [local(x, r, sem, at) for at, (x, r) in enumerate(zip(s_in, r_s))]
        start_all(loads)
        acc[...] = jnp.zeros(acc.shape, F32)
        at = 0
        for i, layer, _, c, *arrays in pieces:
            mine, at = slice(at, at + len(arrays)), at + len(arrays)
            wait_all(loads[mine])

            def some(m):
                here = chunk(m, 16)
                own, *more = r_s[mine]
                g = own[here, :].astype(F32)
                for x in more:
                    g = g + sum(x[y, here, :].astype(F32) for y in EACH)
                g = g.astype(BF16)
                g_s[i][layer, here, c] = g
                square = g.astype(F32)
                square = square * square
                acc[...] += sum(square[:, 128 * y : 128 * (y + 1)] for y in range(c.size // 128))

            loop(sizes[i][1] // 16, some)
        me = lax.axis_index("dp")
        met(others)

        def copy(m, slot):
            return pltpu.make_async_remote_copy(src_ref=acc, dst_ref=tiles.at[slot], send_sem=send.at[m - 1], recv_sem=recv.at[slot], device_id=peer(m), device_id_type=MESH)

        puts = [local(g, o, out_sem, i) for i, (g, o) in enumerate(zip(g_s, g_out))]
        start_all([*puts, *(copy(m, me) for m in others)])
        tiles[me] = acc[...]
        for m in others:
            copy(m, me).wait_send()
            copy(m, peer(m)["dp"]).wait_recv()
        total = tiles[0]
        for m in others:
            total = total + tiles[m]
        total_out[...] = jnp.broadcast_to(jnp.sum(total, keepdims=True), total.shape)
        wait_all(puts)

    *got, total = pl.pallas_call(
        kernel,
        in_specs=[ANY] * len(sums),
        out_specs=[*[ANY] * n, block(memory_space=VM)],
        out_shape=[*[shape(*z) for z in sizes], shape(16, 128, dtype=F32)],
        scratch_shapes=[*[VM(z, BF16) for z in sizes], *[VM(x.shape, x.dtype) for x in sums], VM((16, 128), F32), VM((16, 16, 128), F32), DMA((len(sums),)),
                        DMA((n,)), DMA((15,)), DMA((16,))],
        compiler_params=pltpu.CompilerParams(vmem_limit_bytes=LIMIT, **talk()),
    )(*sums)
    return got, total


def update(weights, moments, seconds, gradients, total, tiles=8):
    n = len(weights)
    count = 16 * sum(w.size for w in weights)
    flat_all = lambda arrays: [x.reshape(-1, x.shape[-1]) for x in arrays]
    args = [y for x in (weights, moments, seconds, gradients) for y in flat_all(x)]

    def body(total_ref, *refs):
        w_in, m_in, v_in, g_in, w_out, m_out, v_out = (refs[n * i : n * (i + 1)] for i in range(7))
        factor = jnp.minimum(1.0, 0.5 * lax.rsqrt(total_ref[...][:1, :1] / count + 1e-30))
        for i in range(n):
            g, w = g_in[i][...].astype(F32) * factor, w_in[i][...].astype(F32)
            m = 0.9 * m_in[i][...] + 0.1 * g
            v = 0.95 * v_in[i][...] + 0.05 * g * g
            m_out[i][...] = m
            v_out[i][...] = v
            w_out[i][...] = (w - 0.02 * (m * lax.rsqrt(v + 1e-8) + 0.1 * w)).astype(BF16)

    specs = [rows(x.shape[0] // tiles, x.shape[1]) for x in args]
    got = run(body, (tiles,), [total, *args], [once(*total.shape), *specs], specs[: 3 * n], [shape(*x.shape, dtype=x.dtype) for x in args[: 3 * n]])
    return tuple(x.reshape(w.shape) for x, w in zip(got, [*weights] * 3))


def step(x, dy, *arrays):
    weights, moments, seconds = (arrays[i : i + len(arrays) // 3] for i in range(0, len(arrays), len(arrays) // 3))
    wq, wk, wv, wo, gate, up, down = weights
    (*_, wo0, gate0, up0, down0), (*_, wo1, gate1, up1, down1) = ([w[n] for w in weights] for n in range(wq.shape[0]))
    (x,), (dy,) = x, dy
    IDS.clear()
    cos, sin = tables(x.shape[0])
    apart = lambda w: w.reshape(16, -1, w.shape[1])
    gathered = lambda w: lax.all_gather(w, "dp", axis=0, tiled=True)
    project, cut = (wq, wk, wv), 6
    hidden, later = gate0.shape[-1], (0, 3, 3)

    B0 = gathered(jnp.concatenate([gate0, up0, wo0], -1))
    Wd0 = apart(gathered(jnp.concatenate([down0, wo1])))
    B1 = gathered(jnp.concatenate([gate1, up1], -1))
    Wd1 = apart(gathered(down1))
    wo_at = (apart(B0), (0, 2 * hidden // wo.shape[2])), (Wd0, (len(down0) // len(wo1), 0))
    (W0,) = run(None, (1,), [], [], [], [], jobs=[Fetch(project, 0)])
    a0, q0, k0, v0 = qkv(x, W0, cos, sin)
    o0, lse0 = attend(q0, k0, v0)
    h0, b0 = joined(o0, *wo_at[0], x)
    act0, pu0, pg0, W1 = gated(b0, B0, hidden, [Fetch(project, 1, (1, 2, 3, 7))])
    (h1,) = joined(act0, Wd0, (0, 0), h0, norm=False)
    a1, q1, k1, v1 = qkv(h1, W1, cos, sin)
    o1, lse1 = attend(q1, k1, v1)
    h2, b1 = joined(o1, *wo_at[1], h1)
    act1, pu1, pg1 = gated(b1, B1, hidden)

    (Dd1,) = by_weight(act1, dy)
    *_, Dg1, Du1, dh2, _, _, d1q, _, _, g1q, _, _, u1q = mlp_back(dy, b1, B1, Wd1, pu1, pg1, h2, chained([Dd1]), cut)
    do1, Do1, g1p, u1p = projected_back(dh2, o1, *wo_at[1], [Pair([Dg1]), Pair([Du1])])
    halves = Half([Dg1], g1p), Half([Du1], u1p, later)
    dq1, dk1, dv1, *_, e1q, f1q, o1p = attend_back(q1, k1, v1, o1, do1, lse1, cos, sin, [
        *halves, Quad([Dg1], g1p, halves[0], at_once(3)), Quad([Du1], u1p, halves[1], at_once(5)), Pair([Do1])])
    *D1, o1h = by_weights(a1, [dq1, dk1, dv1], [Half([Do1], o1p)], tn=HEAD)
    dh1, o1q, a1p = by_input([dq1, dk1, dv1], [(w, 0) for w in W1], h1, dh2, [Quad([Do1], o1p, o1h), Pair(D1)])

    Dd0, a1h = by_weight(act0, dh1, [Half(D1, a1p)])
    *_, Dg0, Du0, dh0, a1q, _, _, d0q, _, _, g0q, _, _, u0q = mlp_back(dh1, b0, B0, Wd0, pu0, pg0, h0, [Quad(D1, a1p, a1h), *chained([Dd0])], cut)
    do0, Do0, g0p, u0p = projected_back(dh0, o0, *wo_at[0], [Pair([Dg0]), Pair([Du0])])
    halves = Half([Dg0], g0p), Half([Du0], u0p, later)
    dq0, dk0, dv0, _, _, e0q, f0q, o0p, o0h = attend_back(q0, k0, v0, o0, do0, lse0, cos, sin, [
        *halves, Quad([Dg0], g0p, halves[0], at_once(3)), Quad([Du0], u0p, halves[1], at_once(5)), *chained([Do0])[:2]])
    a0s, o0q = last_weights(a0, [dq0, dk0, dv0], [Quad([Do0], o0p, o0h)])

    moved = lambda quad: [(n, pl.ds(c.start + cut * HEAD, c.size), *sums) for n, c, *sums in quad]
    layer0 = [*a0s, o0q, g0q + moved(e0q), u0q + moved(f0q), d0q]
    layer1 = [*([part] for part in a1q), o1q, g1q + moved(e1q), u1q + moved(f1q), d1q]
    return update(weights, moments, seconds, *join(list(zip(layer0, layer1)), [w.shape for w in weights]))


def solution(mesh):
    states, cut = P(("rep", "dp"), None, None), P(None, "dp", None)
    return jax.shard_map(
        step,
        mesh=mesh,
        in_specs=(states, states) + (cut,) * 21,
        out_specs=(P("rep", "dp", None),) * 21,
        check_vma=False,
    )
```

```python
import jax
import jax.numpy as jnp
from jax import lax
from jax.experimental import pallas as pl
from jax.experimental.pallas import tpu as pltpu
from jax.sharding import PartitionSpec as P

F32, BF16 = jnp.float32, jnp.bfloat16
MESH = pl.DeviceIdType.MESH
ANY = pl.BlockSpec(memory_space=pl.ANY)
DMA, VM = pltpu.SemaphoreType.DMA, pltpu.VMEM
LIMIT = 62 * 2**20
WORK = 2 * 10**10
WIDE = 512
HEAD = 256
HEADS = 4
THETA = 10000
LOG2E = 1.4426950408889634
NEG = -1e30
HIDDEN = 2 * NEG
DIMS = (8, 4, 2)
CORE = 1
ALL = slice(None)
EACH = range(3)
CUBE = (2, 2, 2, 2)


def dot(a, b, ca, cb):
    return lax.dot_general(a, b, (((ca,), (cb,)), ((), ())), preferred_element_type=F32)


def nn(a, b):
    return dot(a, b, 1, 0)


def nt(a, b):
    return dot(a, b, 1, 1)


def tt(a, b):
    return dot(a, b, 0, 0)


def shape(*size, dtype=BF16):
    return jax.ShapeDtypeStruct(size, dtype)


def chunk(n, size):
    return pl.ds(pl.multiple_of(n * size, size), size)


def loop(count, what):
    lax.fori_loop(0, count, lambda n, _: what(n), None)


def bit(mask):
    return lax.rem(lax.axis_index("dp") // mask, 2)


def peer(mask):
    at = lax.axis_index("dp")
    for m in (*DIMS, CORE):
        if mask & m:
            at = at + m - 2 * m * bit(m)
    return {"dp": at}


def place():
    return [bit(m) for m in DIMS]


def among(p, at):
    return tuple(at if n == p else ALL for n in EACH)


def parts_of(arrays):
    size = arrays[0].shape[-1]
    if len(arrays) > 1:
        return [(n, pl.ds(0, size)) for n in EACH]
    unit = size // 128
    wide = -(-unit // 3)
    return [(0, pl.ds(128 * wide * n, 128 * min(wide, unit - wide * n))) for n in EACH]


def remote(src, dst, sems, n, mask):
    return pltpu.make_async_remote_copy(src_ref=src, dst_ref=dst, send_sem=sems[0].at[n], recv_sem=sems[1].at[n], device_id=peer(mask), device_id_type=MESH)


def local(src, dst, sems, n):
    return pltpu.make_async_copy(src, dst, sems.at[n])


def start_all(copies):
    for c in copies:
        c.start()


def wait_all(copies):
    for c in copies:
        c.wait()


def flat(ref):
    size = 1
    for n in ref.shape[:-1]:
        size *= n
    return ref.reshape(size, ref.shape[-1])


def added(into, others, size=64):
    into, others = flat(into), [flat(o) for o in others]

    def some(n):
        at = chunk(n, size)
        total = into[at, :].astype(F32)
        for o in others:
            total = total + o[at, :].astype(F32)
        into[at, :] = total.astype(BF16)

    loop(into.shape[0] // size, some)


class Fetch:
    masks = (*DIMS, CORE)

    def __init__(self, ws, layer, at=(1, 3, 5, 7)):
        _, self.rows, self.columns = ws[0].shape
        self.layer, self.at, self.ins, k = layer, at, list(ws), len(ws)
        self.outs = [shape(*CUBE, self.rows, self.columns)] * k
        self.scratch = [VM((k, self.rows, self.columns), BF16), DMA((2 * k,)), DMA((21,)), DMA((21,))]
        self.parts = parts_of(ws)

    def done(self, outs):
        return [o.reshape(16 * self.rows, self.columns) for o in outs]

    def stages(self, ws, fulls, scratch):
        own, sem, *sems = scratch
        b, core, k = place(), bit(CORE), len(ws)
        loads = lambda: [local(w.at[self.layer], own.at[n], sem, n) for n, w in enumerate(ws)]
        keeps = lambda: [local(own.at[n], full.at[(*b, core)], sem, k + n) for n, full in enumerate(fulls)]
        axis = lambda p, level: (p + 2 - level) % 3

        def held(p, level, other=None):
            which, columns = self.parts[p]
            idx = list(b)
            for n in range(level):
                idx[axis(p, n)] = ALL
            if other:
                idx[axis(p, level)] = 1 - b[axis(p, level)]
            return fulls[which].at[(*idx, core, ALL, columns)]

        def first_of(p):
            which, columns = self.parts[p]
            return own.at[which, :, columns]

        def across(p, level):
            return remote(held(p, level) if level else first_of(p), held(p, level), sems, 3 * level + p, DIMS[axis(p, level)])

        def pair(p, level):
            if not level:
                return remote(first_of(p), held(p, level), sems, 9 + p, CORE)
            got = held(p, level - 1, True)
            return remote(got, got, sems, 9 + 3 * level + p, CORE)

        def begin():
            start_all(loads())

        def first():
            wait_all(loads())
            start_all(keeps())
            start_all([across(p, 0) for p in EACH] + [pair(p, 0) for p in EACH])

        def next_of(level):
            def go():
                if level == 1:
                    wait_all(keeps())
                for p in EACH:
                    across(p, level - 1).wait_recv()
                    if level < 3:
                        across(p, level).start()
                    pair(p, level).start()

            return go

        def end():
            for p in EACH:
                for level in EACH:
                    across(p, level).wait_send()
                wait_all([pair(p, level) for level in range(4)])

        return [(0, begin), *zip(self.at, (first, *(next_of(n + 1) for n in EACH))), (None, end)]


def cube(g):
    return g if len(g.shape) > len(CUBE) else g.reshape(*CUBE, g.shape[0] // 16, g.shape[1])


class Mine:
    def __init__(self, index, *size):
        self.index, self.shape = index, size


def given(arrays):
    return [x for x in arrays if not isinstance(x, Mine)] if isinstance(arrays, list) else []


def gradients_of(job, refs):
    n = len(given(job.grads))
    return refs[:n] or [job.outer[g.index] for g in job.grads], refs[n:]


class Pair:
    masks = (CORE,)
    followed = None

    def __init__(self, grads, at=1):
        self.grads = [cube(g) for g in grads]
        self.at, self.ins = at, given(self.grads)
        self.outs = [shape(*CUBE[1:], *g.shape[4:]) for g in self.grads]
        self.scratch = [DMA((len(grads),))] * 2

    def done(self, outs):
        return outs

    def stages(self, ins, outs, sems):
        self.refs = outs
        grads, _ = gradients_of(self, ins)
        self.copies = lambda: [remote(g.at[:, :, :, 1 - bit(CORE)], r, sems, n, CORE) for n, (g, r) in enumerate(zip(grads, outs))]
        return [(self.at, lambda: start_all(self.copies())), (None, lambda: left(self))]


def left(job):
    for c in job.copies():
        if job.followed:
            c.wait_send()
        else:
            c.wait()


def follow(before, refs):
    if isinstance(before, list):
        return refs, lambda: None
    before.followed = True

    def arrive():
        for c in before.copies():
            c.wait_recv()

    return before.refs, arrive


class Half:
    masks = DIMS
    followed = None

    def __init__(self, grads, pairs, at=(0, 1, 1)):
        self.at, self.grads, self.parts, self.pairs = at, [*map(cube, grads)], parts_of(grads), pairs
        self.ins = [*given(self.grads), *given(pairs)]
        self.sizes = [(2, 2, self.grads[0].shape[4], c.size) for _, c in self.parts]
        self.outs = [shape(*s) for s in self.sizes]
        self.scratch = [VM(s, BF16) for s in self.sizes] * 2 + [DMA((6,)), DMA((3,)), DMA((3,))]

    def done(self, outs):
        return outs

    def stages(self, ins, outs, scratch):
        grads, ins = gradients_of(self, ins)
        pairs, arrive = follow(self.pairs, ins)
        a, r, (sem, *sems) = scratch[:3], scratch[3:6], scratch[6:]
        self.refs, self.spare = outs, r

        def loads():
            got = []
            for p, (n, columns) in enumerate(self.parts):
                at = among(p, 1 - bit(DIMS[p]))
                got.append(local(grads[n].at[(*at, bit(CORE), ALL, columns)], a[p], sem, p))
                got.append(local(pairs[n].at[(*at, ALL, columns)], r[p], sem, 3 + p))
            return got

        def begin():
            arrive()
            start_all(loads())

        def add():
            wait_all(loads())
            for p in EACH:
                added(a[p], [r[p]])

        self.copies = lambda: [remote(a[p], outs[p], sems, p, DIMS[p]) for p in EACH]
        return [*zip(self.at, (begin, add, lambda: start_all(self.copies()))), (None, lambda: left(self))]


class Quad:
    masks = (2, 4, 6, 8, 10, 12)

    def __init__(self, grads, pairs, halves, at=(0, 1, 1)):
        self.at, self.grads, self.parts, self.pairs, self.halves = at, [*map(cube, grads)], parts_of(grads), pairs, halves
        self.ins = [*given(self.grads), *given(pairs), *given(halves)]
        rows = self.grads[0].shape[4]
        self.outs = [shape(rows, c.size, dtype=F32) for _, c in self.parts] + [shape(3, rows, c.size) for _, c in self.parts]
        self.scratch = [VM((2, 2, rows, c.size), BF16) for _, c in self.parts] * (3 if given(halves) else 2) + [VM((rows, c.size), F32) for _, c in self.parts]
        self.scratch += [DMA((12,)), DMA((9,)), DMA((9,))]

    def done(self, outs):
        return [(*part, *sums) for part, *sums in zip(self.parts, outs[:3], outs[3:])]

    def stages(self, ins, outs, scratch):
        grads, ins = gradients_of(self, ins)
        m = len(given(self.pairs))
        pairs, _ = follow(self.pairs, ins[:m])
        halves, arrive = follow(self.halves, ins[m:])
        sem, *sems = scratch[-3:]
        a, s, own, r = scratch[:3], scratch[3:6], scratch[-6:-3], getattr(self.halves, "spare", scratch[6:9])

        def loads():
            got = []
            for p, (n, columns) in enumerate(self.parts):
                at = among(p, bit(DIMS[p]))
                got.append(local(grads[n].at[(*at, bit(CORE), ALL, columns)], a[p], sem, p))
                got.append(local(pairs[n].at[(*at, ALL, columns)], r[p], sem, 3 + p))
                got.append(local(halves[p], s[p], sem, 6 + p))
            return got

        def begin():
            arrive()
            start_all(loads())

        def add():
            wait_all(loads())
            for p in EACH:
                total_of(p, own[p], a[p], r[p], s[p])
                added(a[p], [r[p], s[p]])

        copies = lambda: [local(own[p], outs[p], sem, 9 + p) for p in EACH] + [c for p in EACH for c in to_three(p, a[p], outs[3 + p], sems)]
        return [*zip(self.at, (begin, add, lambda: start_all(copies()))), (None, lambda: wait_all(copies()))]


def chained(grads, ready=0, third=4):
    pair = Pair(grads, ready + 1)
    half = Half(grads, pair, at_once(ready + 3))
    return [pair, half, Quad(grads, pair, half, at_once(ready + 3 + third))]


def at_once(n):
    return n, n + 1, n + 1


def sides(p):
    u, v = (n for n in EACH if n != p)
    return u, v, bit(DIMS[u]), bit(DIMS[v])


def total_of(p, own, *terms, size=64):
    _, _, bu, bv = sides(p)

    def some(n):
        at = chunk(n, size)
        own[at, :] = sum(x[bu, bv, at, :].astype(F32) for x in terms)

    loop(own.shape[0] // size, some)


def to_three(p, blocks, others, sems, base=0):
    u, v, bu, bv = sides(p)
    flips = ((1, 0), (0, 1), (1, 1))
    return [remote(blocks.at[1 - bu if fu else bu, 1 - bv if fv else bv], others.at[n], sems, base + 3 * p + n, DIMS[u] * fu + DIMS[v] * fv)
            for n, (fu, fv) in enumerate(flips)]


IDS = []


def talk():
    IDS.append(None)
    return dict(collective_id=len(IDS), has_side_effects=True)


def hello(masks):
    for m in masks:
        pl.semaphore_signal(pltpu.get_barrier_semaphore(), inc=1, device_id=peer(m), device_id_type=MESH)


def met(masks):
    pl.semaphore_wait(pltpu.get_barrier_semaphore(), len(masks))


def run(body, grid, args, in_specs, out_specs, out_shapes, scratch=(), jobs=()):
    steps = 1
    for g in grid:
        steps *= g
    gather = lambda name: [x for job in jobs for x in getattr(job, name)]
    ins, outs, scr = gather("ins"), gather("outs"), gather("scratch")
    masks = sorted(set(gather("masks")))

    def kernel(*refs):
        refs = list(refs)
        take = lambda held, n: [held.pop(0) for _ in range(n)]
        my_in, job_in, my_out, job_out, my_scr, job_scr = (take(refs, len(x)) for x in (args, ins, out_shapes, outs, scratch, scr))
        step = 0
        for axis, g in enumerate(grid):
            step = step * g + pl.program_id(axis)
        plan = {}
        for job in jobs:
            job.outer = my_out
            for at, what in job.stages(take(job_in, len(job.ins)), take(job_out, len(job.outs)), take(job_scr, len(job.scratch))):
                plan.setdefault(at if at is None else min(at, steps - 1), []).append(what)
        last = plan.pop(None, [])
        if jobs:
            plan.setdefault(0, []).insert(0, lambda: hello(masks))
            greet = min(1, steps - 1)
            plan.setdefault(greet, []).insert(1 - greet, lambda: met(masks))
        for at in sorted(plan):

            @pl.when(step == at)
            def _(todo=plan[at]):
                for what in todo:
                    what()

        if body is not None:
            body(*my_in, *my_out, *my_scr)
        if last:

            @pl.when(step == steps - 1)
            def _():
                for what in last:
                    what()

    got = list(pl.pallas_call(
        kernel,
        grid=grid,
        in_specs=[*in_specs, *[ANY] * len(ins)],
        out_specs=[*out_specs, *[ANY] * len(outs)],
        out_shape=[*out_shapes, *outs],
        scratch_shapes=[*scratch, *scr],
        compiler_params=pltpu.CompilerParams(dimension_semantics=("arbitrary",) * len(grid), vmem_limit_bytes=LIMIT, **(talk() if jobs else {})),
        cost_estimate=pl.CostEstimate(flops=WORK, bytes_accessed=sum(x.size * x.dtype.itemsize for x in args), transcendentals=0),
    )(*args, *ins))
    mine = [got.pop(0) for _ in out_shapes]
    return (*mine, *(job.done([got.pop(0) for _ in job.outs]) for job in jobs))


block = pl.BlockSpec


def columns(size, tile, skip=0):
    return block((size, tile), lambda j: (0, j + skip))


def slices(size, tile):
    return [slice(n, n + tile) for n in range(0, size, tile)]


def rows(tile, size):
    return block((tile, size), lambda i: (i, 0))


def once(*size):
    return block(size, lambda *_: (0,) * len(size), pipeline_mode=pl.Buffered(1))


class Sum:
    masks = (CORE, *DIMS, 6, 10, 12)

    def __init__(self, grads, at=(0, 1, 2, 4)):
        self.at, self.ins = at, [*map(cube, grads)]
        self.parts = parts_of(grads)
        self.outs = [shape(*g.shape[4:]) for g in self.ins]
        self.scratch = [VM(g.shape, BF16) for g in self.ins] + chain_scratch(self.ins[0].shape[4], self.parts) + [DMA((len(grads),))]

    def done(self, outs):
        return outs

    def stages(self, ins, outs, scratch):
        held, sem = scratch[: len(ins)], scratch[-1]
        core = bit(CORE)
        mine = lambda: [local(g.at[:, :, :, core], h.at[:, :, :, core], sem, n) for n, (g, h) in enumerate(zip(ins, held))]
        pair, half, quad, end = chain([(ins[n], held[n], outs[n], c) for n, c in self.parts], scratch[len(ins) : -1])

        def loaded():
            wait_all(mine())
            half()

        return [*zip(self.at, (lambda: start_all(mine()), pair, loaded, quad)), (None, end)]


def chain_scratch(rows, parts):
    wide = [c.size for _, c in parts]
    return ([VM((2, 2, 2, rows, w), BF16) for w in wide] + [VM((2, 2, rows, w), BF16) for w in wide] * 2 + [VM((3, rows, w), BF16) for w in wide]
            + [VM((rows, w), F32) for w in wide] + [VM((rows, w), BF16) for w in wide] + [DMA((15,))] * 2 + [DMA((3,))])


def chain(parts, scratch):
    (r, s, t, o, own, res), (send, recv, keep) = [scratch[3 * i : 3 * i + 3] for i in range(6)], scratch[18:]
    core = bit(CORE)

    sems = (send, recv)
    to_core = lambda: [remote(src.at[:, :, :, 1 - core, :, c], r[p], sems, p, CORE) for p, (src, _, _, c) in enumerate(parts)]
    to_next = lambda: [remote(s[p], t[p], sems, 3 + p, DIMS[p]) for p in EACH]
    to_rest = lambda: [c for p in EACH for c in to_three(p, s[p], o[p], sems, 6)]
    keeps = lambda: [local(res[p], out.at[:, c], keep, p) for p, (_, _, out, c) in enumerate(parts)]

    def both(p, place, i, j):
        xyz = [i, j]
        xyz.insert(p, place)
        _, held, _, c = parts[p]
        return held[(*xyz, core, ALL, c)].astype(F32) + r[p][tuple(xyz)].astype(F32)

    def half():
        for c in to_core():
            c.wait_recv()
        for p in EACH:

            def some(n, p=p):
                i, j = n // 2, lax.rem(n, 2)
                s[p][i, j] = both(p, 1 - bit(DIMS[p]), i, j).astype(BF16)

            loop(4, some)
        start_all(to_next())

    def quad():
        for c in to_next():
            c.wait()
        for p in EACH:
            u, v, bu, bv = sides(p)

            def some(n, p=p):
                i, j = n // 2, lax.rem(n, 2)
                s[p][i, j] = (both(p, bit(DIMS[p]), i, j) + t[p][i, j].astype(F32)).astype(BF16)

            own[p][...] = both(p, bit(DIMS[p]), bu, bv) + t[p][bu, bv].astype(F32)
            loop(4, some)
        start_all(to_rest())

    def end():
        for c in to_core():
            c.wait_send()
        wait_all(to_rest())
        for p in EACH:
            res[p][...] = (own[p][...] + sum(o[p][n].astype(F32) for n in EACH)).astype(BF16)
        start_all(keeps())
        wait_all(keeps())

    return lambda: start_all(to_core()), half, quad, end


def unit(h):
    wide = h.astype(F32)
    return wide, lax.rsqrt(jnp.mean(wide * wide, -1, keepdims=True) + 1e-6)


def normed(h):
    wide, scale = unit(h)
    return (wide * scale).astype(BF16)


def unit_back(h, by_normed, by_h):
    wide, scale = unit(h)
    d = by_normed.astype(BF16).astype(F32)
    d = scale * d - wide * (scale * scale * scale * jnp.mean(d * wide, -1, keepdims=True))
    return (by_h.astype(F32) + d.astype(BF16).astype(F32)).astype(BF16)


def turned(t, cos, sin):
    half = t.shape[1] // 2
    a, b = t[:, :half], t[:, half:]
    return jnp.concatenate([a * cos - b * sin, b * cos + a * sin], -1)


def tables(tokens):
    half = HEAD // 2
    angle = jnp.arange(tokens, dtype=F32)[:, None] * THETA ** (-jnp.arange(half, dtype=F32) / half)
    return jnp.cos(angle), jnp.sin(angle)


def head(i):
    return slice(i * HEAD, (i + 1) * HEAD)


def qkv(h, w, cos, sin, jobs=(), tm=HEAD):
    t, d = h.shape
    n = w[0].shape[1]

    def body(h_ref, wq, wk, wv, cos_ref, sin_ref, a_ref, q_ref, k_ref, v_ref):
        a = normed(h_ref[...])
        a_ref[...] = a
        v_ref[...] = nn(a, wv[...]).astype(BF16)
        for w_ref, o_ref in ((wq, q_ref), (wk, k_ref)):
            y = nn(a, w_ref[...]).astype(BF16)
            for i in range(n // HEAD):
                o_ref[:, head(i)] = turned(y[:, head(i)].astype(F32), cos_ref[...], sin_ref[...]).astype(BF16)

    part, angle = rows(tm, n), rows(tm, HEAD // 2)
    return run(body, (t // tm,), [h, *w, cos, sin], [rows(tm, d), *[once(d, n)] * 3, angle, angle], [rows(tm, d), part, part, part],
               [shape(t, d), *[shape(t, n)] * 3], jobs=jobs)


def gap(bk, bq):
    return lax.broadcasted_iota(jnp.int32, (bk, bq), 1) - lax.broadcasted_iota(jnp.int32, (bk, bq), 0)


def blocks_of(iq, bq, bk, one):
    per = bq // bk
    loop(iq * per, lambda j: one(j, None))
    lax.fori_loop(iq * per, iq * per + per, lambda j, _: one(j, j * bk - iq * bq), None)


def attend(q, k, v, jobs=(), bq=WIDE, bk=WIDE, strip=WIDE):
    t, n = q.shape
    scale = HEAD**-0.5
    e = scale * LOG2E
    pieces = [(i, at) for i in range(HEADS) for at in slices(bq, strip)]

    def body(q_ref, k_ref, v_ref, o_ref, lse_ref, top_s, mix_s):
        top_s[...] = jnp.full(top_s.shape, NEG, F32)
        mix_s[...] = jnp.zeros(mix_s.shape, F32)
        ones = jnp.ones((8, bk), BF16)

        def one(j, hidden):
            here = chunk(j, bk)
            scores = [nt(k_ref[here, head(i)], q_ref[at, head(i)]) for i, at in pieces]
            weights, keeps = [], []
            for (i, at), s in zip(pieces, scores):
                if hidden is not None:
                    s = jnp.where(gap(bk, strip) >= hidden - at.start, s, HIDDEN)
                old = top_s[pl.ds(i, 1), at]
                top = jnp.maximum(old, s.max(axis=0, keepdims=True))
                top_s[pl.ds(i, 1), at] = top
                weights.append(jnp.exp2((s - top) * e).astype(BF16))
                keeps.append(jnp.exp2((old - top) * e))
            for (i, at), p, keep in zip(pieces, weights, keeps):
                values = jnp.concatenate([v_ref[here, head(i)].T, ones], axis=0)
                mix_s[i, :, at] = mix_s[i, :, at] * keep + nn(values, p)

        blocks_of(pl.program_id(0), bq, bk, one)
        for i in range(HEADS):
            total = mix_s[i, HEAD : HEAD + 1, :]
            o_ref[:, head(i)] = (mix_s[i, :HEAD, :] * (1 / total)).T.astype(BF16)
            lse_ref[pl.ds(i, 1), :] = top_s[pl.ds(i, 1), :] * scale + jnp.log(total)

    part = rows(bq, n)
    return run(body, (t // bq,), [q, k, v], [part, once(t, n), once(t, n)], [part, columns(HEADS, bq)],
               [shape(t, n), shape(HEADS, t, dtype=F32)], [VM((HEADS, bq), F32), VM((HEADS, HEAD + 8, bq), F32)],
               jobs=jobs)


def attend_back(q, k, v, out, by_out, lse, cos, sin, jobs=(), bq=WIDE, bk=WIDE, strip=WIDE, together=2):
    t, n = q.shape
    scale = HEAD**-0.5
    e = scale * LOG2E
    width = together * HEAD
    nq = t // bq
    pieces = [(i, at) for i in range(together) for at in slices(bq, strip)]

    def back(d, cos, sin):
        return turned(d.astype(BF16).astype(F32), cos, -sin).astype(BF16)

    def body(q_ref, k_ref, v_ref, o_ref, do_ref, lse_ref, cos_ref, sin_ref, dq_ref, dk_ref, dv_ref, dq_s, dk_s, dv_s, lse_s, delta_s):
        first, iq = pl.program_id(0) * together, pl.program_id(1)

        @pl.when(iq == 0)
        def _():
            dk_s[...] = jnp.zeros(dk_s.shape, F32)
            dv_s[...] = jnp.zeros(dv_s.shape, F32)

        dq_s[...] = jnp.zeros(dq_s.shape, F32)
        for i in range(together):
            lse_s[pl.ds(i, 1), :] = lse_ref[pl.ds(first + i, 1), :] * LOG2E
            both = do_ref[:, head(i)].astype(F32) * o_ref[:, head(i)].astype(F32)
            delta_s[pl.ds(i, 1), :] = (both[:, : HEAD // 2] + both[:, HEAD // 2 :]).T.sum(axis=0, keepdims=True)

        def one(j, hidden):
            here = chunk(j, bk)
            scores = [nt(k_ref[here, head(i)], q_ref[at, head(i)]) for i, at in pieces]
            dps = [nt(v_ref[here, head(i)], do_ref[at, head(i)]) for i, at in pieces]
            for (i, at), s, dp in zip(pieces, scores, dps):
                p = jnp.exp2(s * e - lse_s[pl.ds(i, 1), at])
                if hidden is not None:
                    p = jnp.where(gap(bk, strip) >= hidden - at.start, p, 0.0)
                ds = (p * (dp - delta_s[pl.ds(i, 1), at])).astype(BF16)
                dv_s[here, head(i)] += nn(p.astype(BF16), do_ref[at, head(i)])
                dk_s[here, head(i)] += nn(ds, q_ref[at, head(i)])
                dq_s[i, :, at] += nn(k_ref[here, head(i)].T, ds)

        blocks_of(iq, bq, bk, one)
        these = chunk(iq, bq)
        for i in range(together):
            dq_ref[:, head(i)] = back((dq_s[i] * scale).T, cos_ref[these, :], sin_ref[these, :])

        @pl.when(iq == nq - 1)
        def _():
            def some(m):
                at = chunk(m, HEAD)
                for i in range(together):
                    dk_ref[at, head(i)] = back(dk_s[at, head(i)] * scale, cos_ref[at, :], sin_ref[at, :])
                dv_ref[at, :] = dv_s[at, :].astype(BF16)

            loop(t // HEAD, some)

    part = block((bq, width), lambda h, i: (i, h))
    whole = block((t, width), lambda h, i: (0, h))
    angle = once(t, HEAD // 2)
    return run(body, (n // width, nq), [q, k, v, out, by_out, lse, cos, sin],
               [part, whole, whole, part, part, block((HEADS, bq), lambda h, i: (0, i)), angle, angle], [part, whole, whole], [shape(t, n)] * 3,
               [VM((together, HEAD, bq), F32), VM((t, width), F32), VM((t, width), F32), VM((8, bq), F32), VM((8, bq), F32)],
               jobs=jobs)


def joined(a, w, place, h, jobs=(), tm=WIDE, norm=True):
    t, n = h.shape
    k = a.shape[1]

    def body(a_ref, w_ref, h_ref, o_ref, *b_ref):
        y = nn(a_ref[...], w_ref[...].reshape(k, n)).astype(BF16)
        new = (h_ref[...].astype(F32) + y.astype(F32)).astype(BF16)
        o_ref[...] = new
        for ref in b_ref:
            ref[...] = normed(new)

    outs = [rows(tm, n)] * (1 + norm)
    return run(body, (t // tm,), [a, w, h], [rows(tm, k), block((16, k // 16, n), lambda i: (0, *place), pipeline_mode=pl.Buffered(1)), rows(tm, n)], outs, [shape(t, n) for _ in outs], jobs=jobs)


def gated(b, both, n, jobs=(), tn=HEAD, sub=WIDE):
    t, d = b.shape

    def body(b_ref, g_ref, u_ref, act_ref, by_u, by_g):
        for at in slices(t, sub):
            g, u = nn(b_ref[at, :], g_ref[...]), nn(b_ref[at, :], u_ref[...])
            s = jax.nn.sigmoid(g)
            p = g * s
            by_u[at, :] = p
            by_g[at, :] = u * (s + p * (1 - s))
            act_ref[at, :] = (p * u).astype(BF16)

    tile = columns(t, tn)
    return run(body, (n // tn,), [b, both, both], [once(t, d), columns(d, tn), columns(d, tn, n // tn)], [tile] * 3,
               [shape(t, n), shape(t, n, dtype=F32), shape(t, n, dtype=F32)], jobs=jobs)


def mlp_back(by_h, b, both, down, by_u, by_g, h, jobs, cut, tn=HEAD, sub=WIDE):
    t, d = by_h.shape
    n = by_u.shape[1]
    tiles = n // tn
    sizes = [(*CUBE, d // 16, tn * k) for k in (cut, cut, tiles - cut, tiles - cut)]

    def body(dh_ref, b_ref, wg_ref, wu_ref, wd_ref, pu_ref, pg_ref, h_ref, *refs):
        *outs, out, dg_s, du_s, total, mine, up_s, gate_s, sem = refs
        staged = gate_s, up_s
        j = pl.program_id(0)

        def stores(outs, skip):
            return [local(x, o.at[(*[ALL] * 5, chunk(j - skip, tn))], sem, i) for i, (x, o) in enumerate(zip(staged, outs))]

        @pl.when(j == 0)
        def _():
            total[...] = jnp.zeros(total.shape, F32)

        cuts = slices(t, sub)
        for at in cuts:
            da = nt(dh_ref[at, :], wd_ref[0]).astype(BF16).astype(F32)
            du_s[at, :] = (da * pu_ref[at, :]).astype(BF16)
            dg_s[at, :] = (da * pg_ref[at, :]).astype(BF16)
        for at in cuts:
            total[at, :] += nt(dg_s[at, :], wg_ref[...]) + nt(du_s[at, :], wu_ref[...])

        @pl.when(j > 0)
        def _():
            wait_all(stores(outs, j))

        for x, s in zip((dg_s, du_s), staged):
            s[...] = tt(b_ref[...], x[...]).astype(BF16).reshape(s.shape)

        @pl.when(j < cut)
        def _():
            start_all(stores(outs, 0))

        @pl.when(j >= cut)
        def _():
            start_all(stores(outs[2:], cut))

        @pl.when(j == tiles - 1)
        def _():
            def some(m):
                at = chunk(m, tn)
                mine[at, :] = unit_back(h_ref[at, :], total[at, :], dh_ref[at, :])

            loop(t // tn, some)
            last = [local(mine, out, sem, len(outs)), *stores(outs, j)]
            last[0].start()
            wait_all(last)

    tile = columns(t, tn)
    whole = once(t, d)
    return run(body, (tiles,), [by_h, b, both, both, down, by_u, by_g, h],
               [whole, whole, columns(d, tn), columns(d, tn, tiles), block((1, tn, d), lambda j: (j, 0, 0)), tile, tile, whole], [ANY] * 5,
               [*[shape(*s) for s in sizes], shape(t, d)],
               [VM((t, tn), BF16), VM((t, tn), BF16), VM((t, d), F32), VM((t, d), BF16), *[VM((*CUBE, d // 16, tn), BF16)] * 2, DMA((5,))],
               jobs=[*jobs, *(c for i in (0, 1) for c in chained([Mine(i, *sizes[i])], cut))])


def by_weight(a, d, jobs=(), tm=WIDE):
    t, m = a.shape
    n = d.shape[1]

    def body(a_ref, d_ref, o_ref):
        o_ref[...] = tt(a_ref[...], d_ref[...]).astype(BF16)

    return run(body, (m // tm,), [a, d], [columns(t, tm), once(t, n)], [rows(tm, n)], [shape(m, n)], jobs=jobs)


def by_weights(a, ds, jobs=(), tn=WIDE):
    t, m = a.shape
    n = ds[0].shape[1]
    k = len(ds)

    def body(a_ref, *refs):
        for d_ref, o_ref in zip(refs[:k], refs[k:]):
            o_ref[...] = tt(a_ref[...], d_ref[...]).astype(BF16)

    return run(body, (n // tn,), [a, *ds], [once(t, m), *[columns(t, tn)] * k], [columns(m, tn)] * k, [shape(m, n)] * k, jobs=jobs)


def by_input(ds, ws, h, by_h, jobs=(), tm=HEAD):
    t, n = h.shape
    k = len(ds)

    def body(*refs):
        h_ref, dh_ref, o_ref = refs[2 * k :]
        total = sum(nt(d[...], w[...]) for d, w in zip(refs[:k], refs[k : 2 * k]))
        o_ref[...] = unit_back(h_ref[...], total, dh_ref[...])

    specs = [block((n, d.shape[1]), lambda i, skip=skip: (0, skip), pipeline_mode=pl.Buffered(1)) for d, (_, skip) in zip(ds, ws)]
    return run(body, (t // tm,), [*ds, *[w for w, _ in ws], h, by_h], [*[rows(tm, d.shape[1]) for d in ds], *specs, rows(tm, n), rows(tm, n)], [rows(tm, n)],
               [shape(t, n)], jobs=jobs)


def projected_back(by_h, a, w, place, jobs=(), tn=HEAD):
    t, d = by_h.shape
    n = a.shape[1]

    def body(dh_ref, a_ref, w_ref, da_ref, dw_ref):
        da_ref[...] = nt(dh_ref[...], w_ref[...].reshape(tn, d)).astype(BF16)
        dw_ref[...] = tt(a_ref[...], dh_ref[...]).astype(BF16)

    tile = columns(t, tn)
    return run(body, (n // tn,), [by_h, a, w], [once(t, d), tile, block((16 * tn // n, n // 16, d), lambda j: (j, *place))], [tile, rows(tn, d)], [shape(t, n), shape(n, d)], jobs=jobs)


def last_weights(a, ds, jobs=(), tn=WIDE):
    t, m = a.shape
    n = ds[0].shape[1]
    r, k, cut = m // 16, len(ds), n // tn
    steps = k * cut
    masks = Sum.masks
    unit = n // 128
    parts = []
    for turn in range(k):
        wide = [-(-unit // 3)] * 3
        wide[turn] = unit - 2 * wide[turn]
        parts.append([pl.ds(128 * sum(wide[:p]), 128 * wide[p]) for p in EACH])
    sizes = [chain_scratch(r, [(None, c) for c in own]) for own in parts]

    class Chain:
        ins = ()

        def __init__(self):
            self.masks = masks
            self.outs = [shape(r, n)] * k
            self.scratch = [VM((*CUBE, r, n), BF16)] * k + [x for own in sizes for x in own]

        def done(self, outs):
            return outs

        def stages(self, ins, outs, scratch):
            self.held, scratch, self.steps = scratch[:k], scratch[k:], []
            for i in range(k):
                mine = scratch[len(sizes[0]) * i : len(sizes[0]) * (i + 1)]
                self.steps.append(chain([(self.held[i], self.held[i], outs[i], c) for c in parts[i]], mine))
            got = []
            for i, (pair, half, quad, _) in enumerate(self.steps[:-1]):
                at = cut * (i + 1)
                got += [(at, pair), (at + 1, half)] + [(at + 3, quad)] * (at + 3 < steps)
            return [*got, (None, self.rest)]

        def rest(self):
            *_, (_, _, before, _), (pair, half, quad, _) = self.steps
            for what in (pair, before, half, quad, *(s[-1] for s in self.steps)):
                what()

    work = Chain()

    def body(a_ref, *refs):
        j = pl.program_id(0)
        for i in range(k):

            @pl.when(j // cut == i)
            def _(i=i):
                at = chunk(lax.rem(j, cut), tn)
                work.held[i][:, :, :, :, :, at] = tt(a_ref[...], refs[i][...]).astype(BF16).reshape(*CUBE, r, tn)

    specs = [block((t, tn), lambda j, i=i: (0, jnp.clip(j - cut * i, 0, cut - 1))) for i in range(k)]
    return run(body, (steps,), [a, *ds], [once(t, m), *specs], [], [], jobs=[work, *jobs])


def join(gradients, sizes):
    pieces = [(i, layer, *p) for i, of in enumerate(gradients) for layer, g in enumerate(of)
              for p in (g if isinstance(g, list) else [(None, pl.ds(0, sizes[i][2]), g)])]
    sums = []
    for _, _, _, _, *arrays in pieces:
        sums += arrays
    others = range(1, 16)
    n = len(sizes)

    def kernel(*refs):
        refs = list(refs)
        take = lambda n: [refs.pop(0) for _ in range(n)]
        s_in, g_out, (total_out,), g_s, r_s = take(len(sums)), take(n), take(1), take(n), take(len(sums))
        acc, tiles, sem, out_sem, send, recv = refs
        hello(others)
        loads = [local(x, r, sem, at) for at, (x, r) in enumerate(zip(s_in, r_s))]
        start_all(loads)
        acc[...] = jnp.zeros(acc.shape, F32)
        at = 0
        for i, layer, _, c, *arrays in pieces:
            mine, at = slice(at, at + len(arrays)), at + len(arrays)
            wait_all(loads[mine])

            def some(m):
                here = chunk(m, 16)
                own, *more = r_s[mine]
                g = own[here, :].astype(F32)
                for x in more:
                    g = g + sum(x[y, here, :].astype(F32) for y in EACH)
                g = g.astype(BF16)
                g_s[i][layer, here, c] = g
                square = g.astype(F32)
                square = square * square
                acc[...] += sum(square[:, 128 * y : 128 * (y + 1)] for y in range(c.size // 128))

            loop(sizes[i][1] // 16, some)
        me = lax.axis_index("dp")
        met(others)

        def copy(m, slot):
            return pltpu.make_async_remote_copy(src_ref=acc, dst_ref=tiles.at[slot], send_sem=send.at[m - 1], recv_sem=recv.at[slot], device_id=peer(m), device_id_type=MESH)

        puts = [local(g, o, out_sem, i) for i, (g, o) in enumerate(zip(g_s, g_out))]
        start_all([*puts, *(copy(m, me) for m in others)])
        tiles[me] = acc[...]
        for m in others:
            copy(m, me).wait_send()
            copy(m, peer(m)["dp"]).wait_recv()
        total = tiles[0]
        for m in others:
            total = total + tiles[m]
        total_out[...] = jnp.broadcast_to(jnp.sum(total, keepdims=True), total.shape)
        wait_all(puts)

    *got, total = pl.pallas_call(
        kernel,
        in_specs=[ANY] * len(sums),
        out_specs=[*[ANY] * n, block(memory_space=VM)],
        out_shape=[*[shape(*z) for z in sizes], shape(16, 128, dtype=F32)],
        scratch_shapes=[*[VM(z, BF16) for z in sizes], *[VM(x.shape, x.dtype) for x in sums], VM((16, 128), F32), VM((16, 16, 128), F32), DMA((len(sums),)),
                        DMA((n,)), DMA((15,)), DMA((16,))],
        compiler_params=pltpu.CompilerParams(vmem_limit_bytes=LIMIT, **talk()),
    )(*sums)
    return got, total


def update(weights, moments, seconds, gradients, total, tiles=8):
    n = len(weights)
    count = 16 * sum(w.size for w in weights)
    flat_all = lambda arrays: [x.reshape(-1, x.shape[-1]) for x in arrays]
    args = [y for x in (weights, moments, seconds, gradients) for y in flat_all(x)]

    def body(total_ref, *refs):
        w_in, m_in, v_in, g_in, w_out, m_out, v_out = (refs[n * i : n * (i + 1)] for i in range(7))
        factor = jnp.minimum(1.0, 0.5 * lax.rsqrt(total_ref[...][:1, :1] / count + 1e-30))
        for i in range(n):
            g, w = g_in[i][...].astype(F32) * factor, w_in[i][...].astype(F32)
            m = 0.9 * m_in[i][...] + 0.1 * g
            v = 0.95 * v_in[i][...] + 0.05 * g * g
            m_out[i][...] = m
            v_out[i][...] = v
            w_out[i][...] = (w - 0.02 * (m * lax.rsqrt(v + 1e-8) + 0.1 * w)).astype(BF16)

    specs = [rows(x.shape[0] // tiles, x.shape[1]) for x in args]
    got = run(body, (tiles,), [total, *args], [once(*total.shape), *specs], specs[: 3 * n], [shape(*x.shape, dtype=x.dtype) for x in args[: 3 * n]])
    return tuple(x.reshape(w.shape) for x, w in zip(got, [*weights] * 3))


def step(x, dy, *arrays):
    weights, moments, seconds = (arrays[i : i + len(arrays) // 3] for i in range(0, len(arrays), len(arrays) // 3))
    wq, wk, wv, wo, gate, up, down = weights
    (*_, wo0, gate0, up0, down0), (*_, wo1, gate1, up1, down1) = ([w[n] for w in weights] for n in range(wq.shape[0]))
    (x,), (dy,) = x, dy
    IDS.clear()
    cos, sin = tables(x.shape[0])
    apart = lambda w: w.reshape(16, -1, w.shape[1])
    gathered = lambda w: lax.all_gather(w, "dp", axis=0, tiled=True)
    project, cut = (wq, wk, wv), 7
    hidden, later = gate0.shape[-1], (0, 3, 3)

    B0 = gathered(jnp.concatenate([gate0, up0, wo0], -1))
    Wd0 = apart(gathered(jnp.concatenate([down0, wo1])))
    B1 = gathered(jnp.concatenate([gate1, up1], -1))
    Wd1 = apart(gathered(down1))
    wo_at = (apart(B0), (0, 2 * hidden // wo.shape[2])), (Wd0, (len(down0) // len(wo1), 0))
    (W0,) = run(None, (1,), [], [], [], [], jobs=[Fetch(project, 0)])
    a0, q0, k0, v0 = qkv(x, W0, cos, sin)
    o0, lse0 = attend(q0, k0, v0)
    h0, b0 = joined(o0, *wo_at[0], x)
    act0, pu0, pg0, W1 = gated(b0, B0, hidden, [Fetch(project, 1, (2, 4, 6, 14))])
    (h1,) = joined(act0, Wd0, (0, 0), h0, norm=False)
    a1, q1, k1, v1 = qkv(h1, W1, cos, sin)
    o1, lse1 = attend(q1, k1, v1)
    h2, b1 = joined(o1, *wo_at[1], h1)
    act1, pu1, pg1 = gated(b1, B1, hidden)

    (Dd1,) = by_weight(act1, dy)
    *_, Dg1, Du1, dh2, _, _, d1q, _, _, g1q, _, _, u1q = mlp_back(dy, b1, B1, Wd1, pu1, pg1, h2, chained([Dd1]), cut)
    do1, Do1, g1p, u1p = projected_back(dh2, o1, *wo_at[1], [Pair([Dg1]), Pair([Du1])])
    halves = Half([Dg1], g1p), Half([Du1], u1p, later)
    dq1, dk1, dv1, *_, e1q, f1q, o1p = attend_back(q1, k1, v1, o1, do1, lse1, cos, sin, [
        *halves, Quad([Dg1], g1p, halves[0], at_once(3)), Quad([Du1], u1p, halves[1], at_once(5)), Pair([Do1])])
    *D1, o1h = by_weights(a1, [dq1, dk1, dv1], [Half([Do1], o1p)], tn=HEAD)
    dh1, o1q, a1p = by_input([dq1, dk1, dv1], [(w, 0) for w in W1], h1, dh2, [Quad([Do1], o1p, o1h), Pair(D1)])

    Dd0, a1h = by_weight(act0, dh1, [Half(D1, a1p)])
    *_, Dg0, Du0, dh0, a1q, _, _, d0q, _, _, g0q, _, _, u0q = mlp_back(dh1, b0, B0, Wd0, pu0, pg0, h0, [Quad(D1, a1p, a1h), *chained([Dd0])], cut)
    do0, Do0, g0p, u0p = projected_back(dh0, o0, *wo_at[0], [Pair([Dg0]), Pair([Du0])])
    halves = Half([Dg0], g0p), Half([Du0], u0p, later)
    dq0, dk0, dv0, _, _, e0q, f0q, o0p, o0h = attend_back(q0, k0, v0, o0, do0, lse0, cos, sin, [
        *halves, Quad([Dg0], g0p, halves[0], at_once(3)), Quad([Du0], u0p, halves[1], at_once(5)), *chained([Do0])[:2]])
    a0s, o0q = last_weights(a0, [dq0, dk0, dv0], [Quad([Do0], o0p, o0h)])

    moved = lambda quad: [(n, pl.ds(c.start + cut * HEAD, c.size), *sums) for n, c, *sums in quad]
    layer0 = [*a0s, o0q, g0q + moved(e0q), u0q + moved(f0q), d0q]
    layer1 = [*([part] for part in a1q), o1q, g1q + moved(e1q), u1q + moved(f1q), d1q]
    return update(weights, moments, seconds, *join(list(zip(layer0, layer1)), [w.shape for w in weights]))


def solution(mesh):
    states, cut = P(("rep", "dp"), None, None), P(None, "dp", None)
    return jax.shard_map(
        step,
        mesh=mesh,
        in_specs=(states, states) + (cut,) * 21,
        out_specs=(P("rep", "dp", None),) * 21,
        check_vma=False,
    )
```
